128 devices in a mesh: ctx: 8 (over z, y_lo), grp: 4 (over y_hi, core), tp: 4 (over x).
Axes of the slice: x: 4, y: 4 (y_hi: 2, y_lo: 2; y = y_hi * 2 + y_lo), z: 4, core: 2. Of those that a mesh axis runs over, the one named last changes fastest.
Arguments:
- tokens: bfloat16 [16384, 4608], P(('grp', 'ctx')), parts along dimension 0, may hold values from -6 to 6
- token_pos: int32 [16384], P(('grp', 'ctx')), parts along dimension 0, may hold values from 0 to 4095, as said below
- norm_gain: float32 [4608], replicated, may hold values from 0.1 to 1.9
- query_weight: bfloat16 [4608, 4096], P('ctx', 'tp'), may hold values from -0.09375 to 0.09375
- key_weight: bfloat16 [4608, 2048], P('ctx', 'tp'), may hold values from -0.09375 to 0.09375
- value_weight: bfloat16 [4608, 2048], P('ctx', 'tp'), may hold values from -0.09375 to 0.09375
Outputs:
- attended: bfloat16 [16384, 4096], P(('grp', 'ctx'), 'tp'), parts along dimension 0
The draws below stay inside these ranges and needn't reach their ends.
There are 4 independent parts, one for each index of `grp`. The reference program is written for one: setup_inputs(seed, part) draws one part's arguments, and reference() takes and returns one part's arrays. A program takes and returns all parts, laid end to end along the dimension named above; an argument that names none is the same for every part. Nothing has to cross between parts.
Inputs may be any that keep to these rules, and one draw needn't show every extreme that they name: `token_pos`: the 512 rows of each index of ctx form two runs of 256 consecutive ascending positions, each starting at a multiple of 256; every position of the sequence occurs exactly once.
All inputs are finite; a program needn't handle non-finite values.
Results may differ from the reference program's by a relative error of at most 0.0077.
Values may be sent and summed in bfloat16 or wider, within the bound.
A program may use at most 128 MiB of HBM per device.

```python
import jax
import jax.numpy as jnp
from jax import lax

D = 4608
HEADS = 32
KV_HEADS = 16
HEAD_DIM = 128
TOK_DEV = 512
TOKENS = 4096


def draw_token_pos(key, part):
    half = TOK_DEV // 2
    devices = TOKENS // TOK_DEV
    blocks = 2 * devices
    order = jax.random.permutation(jax.random.fold_in(key, 12), blocks).astype(jnp.int32)
    target = (jnp.asarray(part).astype(jnp.int32) % blocks).astype(jnp.int32)
    where_target = jnp.argmax((order == target).astype(jnp.int32)).astype(jnp.int32)
    leading = order[0]
    order = order.at[where_target].set(leading)
    order = order.at[0].set(target)
    starts = order * half
    positions = starts[:, None] + jnp.arange(half, dtype=jnp.int32)[None, :]
    return positions.reshape(-1).astype(jnp.int32)


def levels(own_key, shape, shards, smallest, largest):
    def one(axis_at, shards_of):
        steps = jax.random.uniform(jax.random.fold_in(jax.random.fold_in(own_key, 6), axis_at), (shards_of,), jnp.float32, smallest / len(shards), largest / len(shards))
        return jnp.repeat(jnp.exp(steps), shape[axis_at] // shards_of).reshape((-1,) + (1,) * (len(shape) - axis_at - 1))

    factor_of = one(*shards[0])
    for cut in shards[1:]:
        factor_of = factor_of * one(*cut)
    return factor_of


def normal_values(key, shape, spread, reach, split=(), held_as=jnp.bfloat16):
    result = spread * jax.random.normal(key, shape, jnp.float32)
    if split:
        result = result * levels(key, shape, split, -0.22, 0.18)
    return jnp.clip(result, -reach, reach).astype(held_as)


def setup_inputs(seed: int = 0, part: int = 0) -> dict:
    seeds = jax.random.split(jax.random.key(seed), 7)
    own_keys = jax.random.split(jax.random.fold_in(seeds[6], part), 7)
    tokens = normal_values(own_keys[0], (TOKENS, D), 1.0, 6.0, ((0, 8),))
    token_pos = draw_token_pos(jax.random.fold_in(jax.random.fold_in(seeds[6], part), 71), part)
    norm_gain = jnp.clip(1.0 + 0.18 * jax.random.normal(seeds[2], (D,), jnp.float32), 0.1, 1.9)
    query_weight = normal_values(seeds[3], (D, HEADS * HEAD_DIM), D ** -0.5, 0.09375, ((0, 8), (1, 4)))
    key_weight = normal_values(seeds[4], (D, KV_HEADS * HEAD_DIM), D ** -0.5, 0.09375, ((0, 8), (1, 4)))
    value_weight = normal_values(seeds[5], (D, KV_HEADS * HEAD_DIM), D ** -0.5, 0.09375, ((0, 8), (1, 4)))
    return {"tokens": tokens, "token_pos": token_pos, "norm_gain": norm_gain, "query_weight": query_weight, "key_weight": key_weight, "value_weight": value_weight}


query_scale = 144.0 ** (-0.5)

def rotate(field, positions):
    half = field.shape[-1] // 2
    freq = 10000.0 ** (-jnp.arange(half, dtype=jnp.float32) * 2.0 / field.shape[-1])
    angle = positions.astype(jnp.float32)[:, None] * freq[None, :]
    cosine = jnp.cos(angle)[:, None, :]
    sine = jnp.sin(angle)[:, None, :]
    first = field[..., :half]
    second = field[..., half:]
    return jnp.concatenate([first * cosine - second * sine, second * cosine + first * sine], -1)

def reference(tokens, token_pos, norm_gain, query_weight, key_weight, value_weight):
    count = tokens.shape[0]
    inputs = tokens.astype(jnp.float32)
    normed = (inputs * lax.rsqrt(lax.optimization_barrier(jnp.mean(inputs * inputs, -1, keepdims=True)) + 1e-06) * norm_gain[None, :]).astype(jnp.bfloat16)
    queries = jnp.dot(normed, query_weight, preferred_element_type=jnp.float32).reshape(count, HEADS, HEAD_DIM)
    queries = (rotate(queries, token_pos) * query_scale).astype(jnp.bfloat16)
    keys = jnp.dot(normed, key_weight, preferred_element_type=jnp.float32).reshape(count, KV_HEADS, HEAD_DIM)
    keys = rotate(keys, token_pos).astype(jnp.bfloat16)
    values = jnp.dot(normed, value_weight, preferred_element_type=jnp.float32).astype(jnp.bfloat16)
    values = values.reshape(count, KV_HEADS, HEAD_DIM)
    key_full = lax.optimization_barrier(keys).astype(jnp.float32)
    value_full = lax.optimization_barrier(values).astype(jnp.float32)
    half = TOK_DEV // 2
    query_blocks = queries.reshape(count // half, half, KV_HEADS, 2, HEAD_DIM)
    pos_blocks = token_pos.reshape(count // half, half)

    def block(args):
        query_part, pos_part = args
        query_part = lax.optimization_barrier(query_part).astype(jnp.float32)
        scores = jnp.einsum('ngrd,mgd->grnm', query_part, key_full)
        capped = 50.0 * jnp.tanh(scores / 50.0)
        allowed = token_pos[None, None, None, :] <= pos_part[None, None, :, None]
        weights = jnp.where(allowed, jnp.exp(capped), 0.0).astype(jnp.bfloat16)
        weights = lax.optimization_barrier(weights).astype(jnp.float32)
        numerator = jnp.einsum('grnm,mgd->ngrd', weights, value_full)
        total = lax.optimization_barrier(jnp.sum(weights, -1))
        return (numerator / jnp.transpose(total, (2, 0, 1))[..., None]).astype(jnp.bfloat16)
    attended = lax.map(block, (query_blocks, pos_blocks))
    return attended.reshape(count, HEADS * HEAD_DIM)
```

```python
import functools
import math

import jax
import jax.numpy as jnp
from jax import lax
from jax.experimental import pallas as pl
from jax.experimental.pallas import tpu as pltpu
from jax.sharding import PartitionSpec as P

HEAD_DIM = 128
MESH = pl.DeviceIdType.MESH
query_scale = 144.0 ** (-0.5)
EXP_SCALE = 50.0 * math.log2(math.e)


def project_kernel(
    x_hbm, gain_ref, wq_hbm, wk_hbm, wv_hbm, cos_ref, sin_ref,
    q_ref, k_ref, v_ref,
    xv, normed, wbuf, acc, local_sem, send_sem, recv_sem,
):
    ctx = lax.axis_index("ctx")
    grp = lax.axis_index("grp")
    z, par = ctx // 2, ctx % 2
    y_hi, core = grp // 2, grp % 2
    up, down, far = (z + 1) % 4, (z + 3) % 4, (z + 2) % 4
    other = 1 - par
    to_up = {"ctx": up * 2 + par}
    to_down = {"ctx": down * 2 + par}
    to_pair = {"ctx": z * 2 + other}
    to_cross = {"ctx": z * 2 + other, "grp": (1 - y_hi) * 2 + core}
    to_peer = {"grp": y_hi * 2 + (1 - core)}
    everyone = (to_up, to_down, to_pair, to_cross, to_peer)

    rows, feats = xv.shape
    depth = wbuf.shape[1]
    quarter = depth // 4
    a, b = core * 2, core * 2 + 1
    pa, pb = (1 - core) * 2, (1 - core) * 2 + 1
    nq, nk = wq_hbm.shape[1], wk_hbm.shape[1]

    barrier = pltpu.get_barrier_semaphore()
    for dev in everyone:
        pl.semaphore_signal(barrier, inc=1, device_id=dev, device_id_type=MESH)
    loads = [
        pltpu.make_async_copy(wq_hbm, wbuf.at[ctx, :, pl.ds(0, nq)], local_sem.at[0]),
        pltpu.make_async_copy(wk_hbm, wbuf.at[ctx, :, pl.ds(nq, nk)], local_sem.at[1]),
        pltpu.make_async_copy(wv_hbm, wbuf.at[ctx, :, pl.ds(nq + nk, nk)], local_sem.at[2]),
        pltpu.make_async_copy(x_hbm, xv, local_sem.at[3]),
    ]
    for load in loads:
        load.start()
    for load in loads[:3]:
        load.wait()
    pl.semaphore_wait(barrier, len(everyone))

    sends = []

    def piece(shard, part):
        return wbuf.at[shard, pl.ds(pl.multiple_of(part * quarter, 16), quarter), :]

    def send(shard, part, *targets):
        for dev in targets:
            copy = pltpu.make_async_remote_copy(
                src_ref=piece(shard, part), dst_ref=piece(shard, part),
                send_sem=send_sem.at[len(sends)], recv_sem=recv_sem.at[shard, part],
                device_id=dev, device_id_type=MESH,
            )
            copy.start()
            sends.append(copy)

    def arrived(shard, part):
        pltpu.make_async_remote_copy(
            src_ref=piece(shard, part), dst_ref=piece(shard, part),
            send_sem=send_sem.at[0], recv_sem=recv_sem.at[shard, part],
            device_id=to_peer, device_id_type=MESH,
        ).wait_recv()

    def add(shard, first=False):
        tile = 256

        @pl.loop(0, wbuf.shape[2] // tile)
        def _(j):
            cols = pl.ds(pl.multiple_of(j * tile, tile), tile)
            part = jnp.dot(normed[shard], wbuf[shard, :, cols], preferred_element_type=jnp.float32)
            acc[:, cols] = part if first else acc[:, cols] + part

    own = ctx
    send(own, a, to_up, to_pair)
    send(own, b, to_down, to_cross)
    send(own, b, to_up)
    send(own, a, to_down)

    loads[3].wait()

    block = 64

    @pl.loop(0, rows // block)
    def _(i):
        at = pl.ds(pl.multiple_of(i * block, block), block)
        value = xv[at, :].astype(jnp.float32)
        scale = lax.rsqrt(jnp.mean(value * value, -1, keepdims=True) + 1e-06)
        out = (value * scale * gain_ref[...]).astype(jnp.bfloat16)
        for s in range(8):
            normed[s, at, :] = out[:, s * depth : (s + 1) * depth]

    add(own, True)

    s_pair = z * 2 + other
    up_own, up_oth = up * 2 + par, up * 2 + other
    down_own, down_oth = down * 2 + par, down * 2 + other
    far_own, far_oth = far * 2 + par, far * 2 + other

    arrived(down_own, a)
    send(down_own, a, to_up, to_pair, to_peer)
    arrived(up_own, b)
    send(up_own, b, to_down, to_cross, to_peer)
    arrived(s_pair, a)
    send(s_pair, a, to_peer)
    arrived(s_pair, b)
    send(s_pair, b, to_peer)
    arrived(s_pair, pa)
    arrived(s_pair, pb)
    add(s_pair)

    arrived(down_own, b)
    send(down_own, b, to_cross, to_peer)
    arrived(up_own, a)
    send(up_own, a, to_pair, to_peer)
    arrived(down_oth, a)
    send(down_oth, a, to_peer)
    arrived(up_oth, b)
    send(up_oth, b, to_peer)
    for s in (down_own, up_own):
        arrived(s, pa)
        arrived(s, pb)
        add(s)

    arrived(far_own, a)
    send(far_own, a, to_pair, to_peer)
    arrived(far_own, b)
    send(far_own, b, to_cross, to_peer)
    arrived(up_oth, a)
    send(up_oth, a, to_peer)
    arrived(down_oth, b)
    send(down_oth, b, to_peer)
    for s in (down_oth, up_oth, far_own):
        arrived(s, pa)
        arrived(s, pb)
        add(s)

    arrived(far_oth, a)
    send(far_oth, a, to_peer)
    arrived(far_oth, b)
    send(far_oth, b, to_peer)
    arrived(far_oth, pa)
    arrived(far_oth, pb)
    add(far_oth)

    half = HEAD_DIM // 2

    def rope(u):
        return u * cos_ref[...] + pltpu.roll(u, half, 1) * sin_ref[...]

    for h in range(nq // HEAD_DIM):
        at = slice(h * HEAD_DIM, (h + 1) * HEAD_DIM)
        q_ref[:, at] = (rope(acc[:, at]) * query_scale).astype(jnp.bfloat16)
    for h in range(nk // HEAD_DIM):
        at = slice(h * HEAD_DIM, (h + 1) * HEAD_DIM)
        k_ref[:, at] = rope(acc[:, nq + h * HEAD_DIM : nq + (h + 1) * HEAD_DIM]).astype(jnp.bfloat16)
    v_ref[...] = acc[:, nq + nk :].astype(jnp.bfloat16)

    for copy in sends:
        copy.wait_send()


def project(tokens, norm_gain, query_weight, key_weight, value_weight, cosine, sine):
    rows, feats = tokens.shape
    depth, nq = query_weight.shape
    nk = key_weight.shape[1]
    vmem = pl.BlockSpec(memory_space=pltpu.VMEM)
    hbm = pl.BlockSpec(memory_space=pl.ANY)
    return pl.pallas_call(
        project_kernel,
        out_shape=(
            jax.ShapeDtypeStruct((rows, nq), jnp.bfloat16),
            jax.ShapeDtypeStruct((rows, nk), jnp.bfloat16),
            jax.ShapeDtypeStruct((rows, nk), jnp.bfloat16),
        ),
        in_specs=[hbm, vmem, hbm, hbm, hbm, vmem, vmem],
        out_specs=(vmem, vmem, vmem),
        scratch_shapes=[
            pltpu.VMEM((rows, feats), jnp.bfloat16),
            pltpu.VMEM((feats // depth, rows, depth), jnp.bfloat16),
            pltpu.VMEM((feats // depth, depth, nq + 2 * nk), jnp.bfloat16),
            pltpu.VMEM((rows, nq + 2 * nk), jnp.float32),
            pltpu.SemaphoreType.DMA((4,)),
            pltpu.SemaphoreType.DMA((28,)),
            pltpu.SemaphoreType.DMA((8, 4)),
        ],
        compiler_params=pltpu.CompilerParams(
            collective_id=0, has_side_effects=True, vmem_limit_bytes=60 * 1024 * 1024
        ),
        name="project",
    )(tokens, norm_gain.reshape(1, feats), query_weight, key_weight, value_weight, cosine, sine)


def attend_kernel(kstart, qstart, q_ref, k_ref, v_ref, qpos_ref, kpos_ref, o_ref, vext, num):
    rows = q_ref.shape[0]
    run = rows // 2
    keys = k_ref.shape[0]
    vext[:, :HEAD_DIM] = v_ref[...]
    vext[:, HEAD_DIM:] = jnp.ones((keys, HEAD_DIM), jnp.bfloat16)
    for r in range(2):
        at = slice(r * run, (r + 1) * run)
        qs = [q_ref[at, h * HEAD_DIM : (h + 1) * HEAD_DIM] for h in range(2)]
        qp = qpos_ref[at, :]
        num[...] = jnp.zeros_like(num)

        def step(masked, kb):
            kat = pl.ds(pl.multiple_of(kb * run, run), run)
            kk = k_ref[kat, :]
            vv = vext[kat, :]
            for h in range(2):
                s = lax.dot_general(qs[h], kk, (((1,), (1,)), ((), ())), preferred_element_type=jnp.float32)
                w = jnp.exp2(jnp.tanh(s * 0.02) * EXP_SCALE)
                if masked:
                    w = jnp.where(kpos_ref[:, kat] <= qp, w, 0.0)
                num[h * run : (h + 1) * run, :] += jnp.dot(
                    w.astype(jnp.bfloat16), vv, preferred_element_type=jnp.float32
                )

        @pl.loop(0, keys // run)
        def _(kb):
            @pl.when(kstart[kb] < qstart[r])
            def _():
                step(False, kb)

            @pl.when(kstart[kb] == qstart[r])
            def _():
                step(True, kb)

        for h in range(2):
            n = num[h * run : (h + 1) * run, :]
            o_ref[at, h * HEAD_DIM : (h + 1) * HEAD_DIM] = (
                n[:, :HEAD_DIM] / n[:, HEAD_DIM:]
            ).astype(jnp.bfloat16)


def attend(queries, key_rows, value_rows, token_pos, key_pos):
    rows, nq = queries.shape
    keys, nk = key_rows.shape
    run = rows // 2
    kv_heads = nk // HEAD_DIM
    return pl.pallas_call(
        attend_kernel,
        out_shape=jax.ShapeDtypeStruct((rows, nq), jnp.bfloat16),
        grid_spec=pltpu.PrefetchScalarGridSpec(
            num_scalar_prefetch=2,
            grid=(kv_heads,),
            in_specs=[
                pl.BlockSpec((rows, 2 * HEAD_DIM), lambda g, *_: (0, g)),
                pl.BlockSpec((keys, HEAD_DIM), lambda g, *_: (0, g)),
                pl.BlockSpec((keys, HEAD_DIM), lambda g, *_: (0, g)),
                pl.BlockSpec((rows, 1), lambda g, *_: (0, 0)),
                pl.BlockSpec((1, keys), lambda g, *_: (0, 0)),
            ],
            out_specs=pl.BlockSpec((rows, 2 * HEAD_DIM), lambda g, *_: (0, g)),
            scratch_shapes=[
                pltpu.VMEM((keys, 2 * HEAD_DIM), jnp.bfloat16),
                pltpu.VMEM((2 * run, 2 * HEAD_DIM), jnp.float32),
            ],
        ),
        compiler_params=pltpu.CompilerParams(vmem_limit_bytes=48 * 1024 * 1024),
        name="attend",
    )(key_pos[::run], token_pos[::run], queries, key_rows, value_rows, token_pos[:, None], key_pos[None, :])


def on_device(tokens, token_pos, norm_gain, query_weight, key_weight, value_weight):
    half = HEAD_DIM // 2
    freq = 10000.0 ** (-jnp.arange(half, dtype=jnp.float32) * 2.0 / HEAD_DIM)
    angle = token_pos.astype(jnp.float32)[:, None] * freq[None, :]
    cosine, sine = jnp.cos(angle), jnp.sin(angle)
    cosine = jnp.concatenate([cosine, cosine], -1)
    sine = jnp.concatenate([-sine, sine], -1)
    queries, keys, values = project(
        tokens, norm_gain, query_weight, key_weight, value_weight, cosine, sine
    )
    both = lax.all_gather(jnp.concatenate([keys, values], 1), "ctx", axis=0, tiled=True)
    nk = keys.shape[1]
    key_pos = lax.all_gather(token_pos, "ctx", axis=0, tiled=True)
    return attend(queries, both[:, :nk], both[:, nk:], token_pos, key_pos)


def solution(mesh):
    in_specs = (
        P(("grp", "ctx"), None),
        P(("grp", "ctx")),
        P(),
        P("ctx", "tp"),
        P("ctx", "tp"),
        P("ctx", "tp"),
    )
    out_specs = P(("grp", "ctx"), "tp")
    return jax.shard_map(
        on_device, mesh=mesh, in_specs=in_specs, out_specs=out_specs, check_vma=False
    )
```

```python
import functools
import math

import jax
import jax.numpy as jnp
from jax import lax
from jax.experimental import pallas as pl
from jax.experimental.pallas import tpu as pltpu
from jax.sharding import PartitionSpec as P

HEAD_DIM = 128
MESH = pl.DeviceIdType.MESH
query_scale = 144.0 ** (-0.5)
EXP_SCALE = 50.0 * math.log2(math.e)
SHARDS = 8
SPLIT_KV = 144
SPLIT_Q = 112


def tile(index, size):
    return pl.ds(pl.multiple_of(index * size, size), size)


def kernel(
    x_hbm, gain_ref, wq_hbm, wk_hbm, wv_hbm, cos_ref, sin_ref, pos_ref,
    o_ref,
    xv, normed, wkv, wq, acc, posb, qpos, kvb, kvx, qb, qx, num, osend, orecv,
    local_sem, send_sem, wkv_sem, wq_sem, kv_sem, q_sem, o_sem, pos_sem,
):
    ctx = lax.axis_index("ctx")
    grp = lax.axis_index("grp")
    z, par = ctx // 2, ctx % 2
    y_hi, core = grp // 2, grp % 2
    up, down, far = (z + 1) % 4, (z + 3) % 4, (z + 2) % 4
    other = 1 - par
    pair = z * 2 + other
    to_up = {"ctx": up * 2 + par}
    to_down = {"ctx": down * 2 + par}
    to_pair = {"ctx": pair}
    to_cross = {"ctx": pair, "grp": (1 - y_hi) * 2 + core}
    to_peer = {"grp": y_hi * 2 + (1 - core)}
    group = [{"ctx": (ctx + i) % SHARDS} for i in range(1, SHARDS)]

    rows, feats = xv.shape
    depth = wq.shape[1]
    nq, nk = wq_hbm.shape[1], wk_hbm.shape[1]
    hd = HEAD_DIM
    half_rows = rows // 2

    barrier = pltpu.get_barrier_semaphore()
    for dev in group + [to_cross, to_peer]:
        pl.semaphore_signal(barrier, inc=1, device_id=dev, device_id_type=MESH)
    loads = [
        pltpu.make_async_copy(wk_hbm, wkv.at[ctx, :, pl.ds(0, nk)], local_sem.at[0]),
        pltpu.make_async_copy(wv_hbm, wkv.at[ctx, :, pl.ds(nk, nk)], local_sem.at[1]),
        pltpu.make_async_copy(x_hbm, xv, local_sem.at[2]),
        pltpu.make_async_copy(wq_hbm, wq.at[ctx], local_sem.at[3]),
    ]
    for load in loads:
        load.start()
    loads[0].wait()
    loads[1].wait()
    pl.semaphore_wait(barrier, SHARDS + 1)

    sends = []

    def copy_of(src, dst, recv, dev, at):
        return pltpu.make_async_remote_copy(
            src_ref=src, dst_ref=dst, send_sem=send_sem.at[at], recv_sem=recv,
            device_id=dev, device_id_type=MESH,
        )

    def send(src, dst, recv, dev):
        copy = copy_of(src, dst, recv, dev, len(sends))
        copy.start()
        sends.append(copy)

    def await_copy(dst, recv):
        copy_of(dst, dst, recv, to_peer, 0).wait_recv()

    class Gather:
        def __init__(self, buf, sem, split):
            self.buf, self.sem, self.split = buf, sem, split

        def piece(self, shard, owner, kind):
            base = owner * (depth // 2) + (self.split if kind else 0)
            size = depth // 2 - self.split if kind else self.split
            return self.buf.at[shard, pl.ds(pl.multiple_of(base, 16), size), :]

        def send(self, shard, kind, *devs):
            ref = self.piece(shard, core, kind)
            for dev in devs:
                send(ref, ref, self.sem.at[shard, core * 2 + kind], dev)

        def wait(self, shard, kind, owner=core):
            await_copy(self.piece(shard, owner, kind), self.sem.at[shard, owner * 2 + kind])

        def relay(self, shard, kind, *devs):
            self.wait(shard, kind)
            self.send(shard, kind, *devs)

        def complete(self, *shards):
            for s in shards:
                self.wait(s, 0, 1 - core)
                self.wait(s, 1, 1 - core)

    A, B = 0, 1
    own = ctx
    up_own, up_oth = up * 2 + par, up * 2 + other
    down_own, down_oth = down * 2 + par, down * 2 + other
    far_own, far_oth = far * 2 + par, far * 2 + other

    gkv = Gather(wkv, wkv_sem, SPLIT_KV)
    gq = Gather(wq, wq_sem, SPLIT_Q)

    def add(buf, shard, at, first=False):
        width = 256

        @pl.loop(0, buf.shape[2] // width)
        def _(j):
            cols = tile(j, width)
            part = jnp.dot(normed[shard], buf[shard, :, cols], preferred_element_type=jnp.float32)
            acc[at, :, cols] = part if first else acc[at, :, cols] + part

    def add_kv(*shards, first=False):
        for s in shards:
            add(wkv, s, 0, first)

    def add_q(*shards, first=False):
        for s in shards:
            add(wq, s, 1, first)

    gkv.send(own, A, to_up, to_pair)
    gkv.send(own, B, to_down, to_cross)
    gkv.send(own, B, to_up)
    gkv.send(own, A, to_down)
    for dev in group:
        send(pos_ref, posb.at[ctx], pos_sem.at[ctx], dev)
    posb[ctx] = pos_ref[...]

    loads[2].wait()
    block = 64

    @pl.loop(0, rows // block)
    def _(i):
        at = tile(i, block)
        value = xv[at, :].astype(jnp.float32)
        scale = lax.rsqrt(jnp.mean(value * value, -1, keepdims=True) + 1e-06)
        out = (value * scale * gain_ref[...]).astype(jnp.bfloat16)
        for s in range(SHARDS):
            normed[s, at, :] = out[:, s * depth : (s + 1) * depth]

    loads[3].wait()
    add_kv(own, first=True)

    gkv.relay(down_own, A, to_up, to_pair, to_peer)
    gkv.relay(up_own, B, to_down, to_cross, to_peer)
    gkv.relay(pair, A, to_peer)
    gkv.relay(pair, B, to_peer)
    gkv.complete(pair)
    add_kv(pair)

    gkv.relay(down_own, B, to_cross, to_peer)
    gkv.relay(up_own, A, to_pair, to_peer)
    gq.send(own, A, to_up)
    gq.send(own, B, to_down)
    gq.send(own, B, to_up)
    gq.send(own, A, to_down)
    gkv.relay(down_oth, A, to_peer)
    gkv.relay(up_oth, B, to_peer)
    gkv.complete(down_own, up_own)
    add_kv(down_own, up_own)

    gkv.relay(far_own, A, to_pair, to_peer)
    gkv.relay(far_own, B, to_cross, to_peer)
    gq.send(own, A, to_pair)
    gq.send(own, B, to_cross)
    gkv.relay(up_oth, A, to_peer)
    gkv.relay(down_oth, B, to_peer)
    gkv.complete(down_oth, up_oth, far_own)
    add_kv(down_oth, up_oth, far_own)
    add_q(own, first=True)

    gkv.relay(far_oth, A, to_peer)
    gkv.relay(far_oth, B, to_peer)
    gq.relay(down_own, A, to_up, to_peer)
    gq.relay(up_own, B, to_down, to_cross, to_peer)
    gkv.complete(far_oth)
    add_kv(far_oth)

    def rope(u):
        return u * cos_ref[...] + pltpu.roll(u, hd // 2, 1) * sin_ref[...]

    for h in range(2):
        for ref, base in ((kvb.at[ctx], par * 2), (kvx, other * 2)):
            ref[:, h * hd : (h + 1) * hd] = rope(acc[0, :, tile(base + h, hd)]).astype(jnp.bfloat16)
            ref[:, (2 + h) * hd : (3 + h) * hd] = acc[0, :, tile(nk // hd + base + h, hd)].astype(
                jnp.bfloat16
            )

    def kv_half(ref, half):
        return ref.at[pl.ds(half * half_rows, half_rows), :]

    def kv_send(src, blk, half, dev):
        send(kv_half(src, half), kv_half(kvb.at[blk], half), kv_sem.at[blk, half], dev)

    def kv_wait(blk, half):
        await_copy(kv_half(kvb.at[blk], half), kv_sem.at[blk, half])

    for half in range(2):
        kv_send(kvx, ctx, half, to_pair)
    for half in range(2):
        kv_send(kvb.at[ctx], ctx, half, to_up)
        kv_send(kvb.at[ctx], ctx, 1 - half, to_down)
    gq.send(down_own, A, to_pair)

    gq.relay(down_own, B, to_cross, to_peer)
    gq.relay(up_own, A, to_pair, to_peer)
    gq.relay(pair, A, to_peer)
    gq.relay(pair, B, to_peer)
    gq.complete(down_own, up_own)
    add_q(down_own, up_own)
    gq.relay(far_own, A, to_pair, to_peer)
    gq.relay(far_own, B, to_cross, to_peer)
    gq.complete(pair)
    add_q(pair)
    kv_wait(pair, 0)
    kv_send(kvb.at[pair], pair, 0, to_up)
    kv_wait(pair, 1)
    kv_send(kvb.at[pair], pair, 1, to_down)
    kv_send(kvb.at[pair], pair, 1, to_up)
    kv_send(kvb.at[pair], pair, 0, to_down)
    gq.relay(down_oth, A, to_peer)
    gq.relay(up_oth, B, to_peer)
    gq.complete(far_own)
    add_q(far_own)
    kv_wait(down_own, 0)
    kv_send(kvb.at[down_own], down_own, 0, to_up)
    kv_wait(up_own, 1)
    kv_send(kvb.at[up_own], up_own, 1, to_down)
    kv_wait(down_own, 1)
    kv_wait(up_own, 0)
    gq.relay(up_oth, A, to_peer)
    gq.relay(down_oth, B, to_peer)
    gq.complete(down_oth, up_oth)
    add_q(down_oth, up_oth)
    gq.relay(far_oth, A, to_peer)
    gq.relay(far_oth, B, to_peer)
    gq.complete(far_oth)
    add_q(far_oth)

    for j in range(2):
        for r in range(2):
            at = slice(r * rows, (r + 1) * rows)
            for ref, base in ((qx, other * 4), (qb.at[0], par * 4)):
                ref[j, at, :] = (rope(acc[1, :, tile(base + 2 * j + r, hd)]) * query_scale).astype(
                    jnp.bfloat16
                )
        send(qx.at[j], qb.at[1, j], q_sem.at[j], to_pair)

    kv_wait(down_oth, 0)
    kv_send(kvb.at[down_oth], down_oth, 0, to_up)
    kv_wait(up_oth, 1)
    kv_send(kvb.at[up_oth], up_oth, 1, to_down)
    kv_wait(down_oth, 1)
    kv_wait(up_oth, 0)

    for i in range(1, SHARDS):
        blk = (ctx + SHARDS - i) % SHARDS
        await_copy(posb.at[blk], pos_sem.at[blk])
    for src, blk in ((0, ctx), (1, pair)):
        col = jnp.transpose(posb[blk])[:, :1]
        for r in range(2):
            qpos[src, r * rows : (r + 1) * rows, :] = col

    def unit(src, j, step, first):
        zr = (z + step + step // 2 - 2 * (step // 3)) % 4
        blocks = pl.ds(zr * 2, 2)
        kk = kvb[blocks, :, tile(j, hd)].reshape(2 * rows, hd)
        vv = kvb[blocks, :, tile(2 + j, hd)].reshape(2 * rows, hd)
        vv = jnp.concatenate([vv, jnp.ones_like(vv)], 1)
        kp = jnp.concatenate([posb[zr * 2, :1, :], posb[zr * 2 + 1, :1, :]], 1)
        s = lax.dot_general(
            qb[src, j], kk, (((1,), (1,)), ((), ())), preferred_element_type=jnp.float32
        )
        w = jnp.exp2(jnp.tanh(s * 0.02) * EXP_SCALE)
        w = jnp.where(kp <= qpos[src], w, 0.0).astype(jnp.bfloat16)
        part = jnp.dot(w, vv, preferred_element_type=jnp.float32)
        num[src, j] = part if first else num[src, j] + part

    def result(src, j, r):
        n = num[src, j, r * rows : (r + 1) * rows, :]
        return (n[:, :hd] / n[:, hd:]).astype(jnp.bfloat16)

    num[...] = jnp.zeros_like(num)

    @pl.loop(0, 2)
    def _(j):
        @pl.loop(0, 3)
        def _(i):
            unit(0, j, i, False)

    for j in range(2):
        await_copy(qb.at[1, j], q_sem.at[j])
        if j == 0:
            for blk in (far_own, far_oth):
                kv_wait(blk, 0)
                kv_wait(blk, 1)

        @pl.loop(0, 4)
        def _(i):
            unit(1, j, i, False)

        for r in range(2):
            osend[2 * j + r] = result(1, j, r)
            send(osend.at[2 * j + r], orecv.at[2 * j + r], o_sem.at[2 * j + r], to_pair)

    @pl.loop(0, 2)
    def _(j):
        unit(0, j, 3, False)

    for j in range(2):
        for r in range(2):
            o_ref[:, tile(par * 4 + 2 * j + r, hd)] = result(0, j, r)
    for h in range(4):
        await_copy(orecv.at[h], o_sem.at[h])
        o_ref[:, tile(other * 4 + h, hd)] = orecv[h]

    for copy in sends:
        copy.wait_send()


def on_device(tokens, token_pos, norm_gain, query_weight, key_weight, value_weight):
    rows, feats = tokens.shape
    depth, nq = query_weight.shape
    nk = key_weight.shape[1]
    half = HEAD_DIM // 2
    freq = 10000.0 ** (-jnp.arange(half, dtype=jnp.float32) * 2.0 / HEAD_DIM)
    position = token_pos.astype(jnp.float32)
    angle = position[:, None] * freq[None, :]
    cosine, sine = jnp.cos(angle), jnp.sin(angle)
    cosine = jnp.concatenate([cosine, cosine], -1)
    sine = jnp.concatenate([-sine, sine], -1)
    vmem = pl.BlockSpec(memory_space=pltpu.VMEM)
    hbm = pl.BlockSpec(memory_space=pl.ANY)
    bf16, f32 = jnp.bfloat16, jnp.float32
    dma = pltpu.SemaphoreType.DMA
    return pl.pallas_call(
        kernel,
        out_shape=jax.ShapeDtypeStruct((rows, nq), bf16),
        in_specs=[hbm, vmem, hbm, hbm, hbm, vmem, vmem, vmem],
        out_specs=vmem,
        scratch_shapes=[
            pltpu.VMEM((rows, feats), bf16),
            pltpu.VMEM((SHARDS, rows, depth), bf16),
            pltpu.VMEM((SHARDS, depth, 2 * nk), bf16),
            pltpu.VMEM((SHARDS, depth, nq), bf16),
            pltpu.VMEM((2, rows, nq), f32),
            pltpu.VMEM((SHARDS, 8, rows), f32),
            pltpu.VMEM((2, 2 * rows, 1), f32),
            pltpu.VMEM((SHARDS, rows, nk), bf16),
            pltpu.VMEM((rows, nk), bf16),
            pltpu.VMEM((2, 2, 2 * rows, HEAD_DIM), bf16),
            pltpu.VMEM((2, 2 * rows, HEAD_DIM), bf16),
            pltpu.VMEM((2, 2, 2 * rows, 2 * HEAD_DIM), f32),
            pltpu.VMEM((4, rows, HEAD_DIM), bf16),
            pltpu.VMEM((4, rows, HEAD_DIM), bf16),
            dma((4,)),
            dma((96,)),
            dma((SHARDS, 4)),
            dma((SHARDS, 4)),
            dma((SHARDS, 2)),
            dma((2,)),
            dma((4,)),
            dma((SHARDS,)),
        ],
        compiler_params=pltpu.CompilerParams(
            collective_id=0, has_side_effects=True, vmem_limit_bytes=62 * 1024 * 1024
        ),
        name="block",
    )(
        tokens, norm_gain.reshape(1, feats), query_weight, key_weight, value_weight,
        cosine, sine, jnp.broadcast_to(position[None, :], (8, rows)),
    )


def solution(mesh):
    in_specs = (
        P(("grp", "ctx"), None),
        P(("grp", "ctx")),
        P(),
        P("ctx", "tp"),
        P("ctx", "tp"),
        P("ctx", "tp"),
    )
    out_specs = P(("grp", "ctx"), "tp")
    return jax.shard_map(
        on_device, mesh=mesh, in_specs=in_specs, out_specs=out_specs, check_vma=False
    )
```

```python
import functools
import math

import jax
import jax.numpy as jnp
from jax import lax
from jax.experimental import pallas as pl
from jax.experimental.pallas import tpu as pltpu
from jax.sharding import PartitionSpec as P

HEAD_DIM = 128
MESH = pl.DeviceIdType.MESH
query_scale = 144.0 ** (-0.5)
EXP_SCALE = 50.0 * math.log2(math.e)
SHARDS = 8
SPLIT_KV = 144
SPLIT_Q = 112


def tile(index, size):
    return pl.ds(pl.multiple_of(index * size, size), size)


def kernel(
    x_hbm, gain_ref, wq_hbm, wk_hbm, wv_hbm, cos_ref, sin_ref, pos_ref,
    o_ref,
    xv, normed, wkv, wq, acc, posb, qpos, kvb, kvx, qb, qx, num, osend, orecv,
    local_sem, send_sem, wkv_sem, wq_sem, kv_sem, q_sem, o_sem, pos_sem,
):
    ctx = lax.axis_index("ctx")
    grp = lax.axis_index("grp")
    z, par = ctx // 2, ctx % 2
    y_hi, core = grp // 2, grp % 2
    up, down, far = (z + 1) % 4, (z + 3) % 4, (z + 2) % 4
    other = 1 - par
    pair = z * 2 + other
    to_up = {"ctx": up * 2 + par}
    to_down = {"ctx": down * 2 + par}
    to_pair = {"ctx": pair}
    to_cross = {"ctx": pair, "grp": (1 - y_hi) * 2 + core}
    to_peer = {"grp": y_hi * 2 + (1 - core)}
    group = [{"ctx": (ctx + i) % SHARDS} for i in range(1, SHARDS)]

    rows, feats = xv.shape
    depth = wkv.shape[1]
    nq, nk = wq_hbm.shape[1], wk_hbm.shape[1]
    hd = HEAD_DIM
    half_rows = rows // 2

    barrier = pltpu.get_barrier_semaphore()
    for dev in group + [to_cross, to_peer]:
        pl.semaphore_signal(barrier, inc=1, device_id=dev, device_id_type=MESH)
    loads = [
        pltpu.make_async_copy(wk_hbm, wkv.at[ctx, :, pl.ds(0, nk)], local_sem.at[0]),
        pltpu.make_async_copy(wv_hbm, wkv.at[ctx, :, pl.ds(nk, nk)], local_sem.at[1]),
        pltpu.make_async_copy(x_hbm, xv, local_sem.at[2]),
    ] + [
        pltpu.make_async_copy(
            wq_hbm.at[:, pl.ds((2 * i + j) * 2 * hd, 2 * hd)],
            wq.at[j, ctx, :, pl.ds(i * 2 * hd, 2 * hd)],
            local_sem.at[3 + 2 * i + j],
        )
        for i in range(2)
        for j in range(2)
    ]
    for load in loads:
        load.start()
    loads[0].wait()
    loads[1].wait()
    pl.semaphore_wait(barrier, SHARDS + 1)

    sends = []

    def copy_of(src, dst, recv, dev, at):
        return pltpu.make_async_remote_copy(
            src_ref=src, dst_ref=dst, send_sem=send_sem.at[at], recv_sem=recv,
            device_id=dev, device_id_type=MESH,
        )

    def send(src, dst, recv, dev):
        copy = copy_of(src, dst, recv, dev, len(sends))
        copy.start()
        sends.append(copy)

    def await_copy(dst, recv):
        copy_of(dst, dst, recv, to_peer, 0).wait_recv()

    class Gather:
        def __init__(self, buf, sem, split):
            self.buf, self.sem, self.split = buf, sem, split

        def piece(self, shard, owner, kind):
            base = owner * (depth // 2) + (self.split if kind else 0)
            size = depth // 2 - self.split if kind else self.split
            return self.buf.at[shard, pl.ds(pl.multiple_of(base, 16), size), :]

        def send(self, shard, kind, *devs):
            ref = self.piece(shard, core, kind)
            for dev in devs:
                send(ref, ref, self.sem.at[shard, core * 2 + kind], dev)

        def wait(self, shard, kind, owner=core):
            await_copy(self.piece(shard, owner, kind), self.sem.at[shard, owner * 2 + kind])

        def relay(self, shard, kind, *devs):
            self.wait(shard, kind)
            self.send(shard, kind, *devs)

        def complete(self, *shards):
            for s in shards:
                self.wait(s, 0, 1 - core)
                self.wait(s, 1, 1 - core)

    A, B = 0, 1
    own = ctx
    up_own, up_oth = up * 2 + par, up * 2 + other
    down_own, down_oth = down * 2 + par, down * 2 + other
    far_own, far_oth = far * 2 + par, far * 2 + other

    gkv = Gather(wkv, wkv_sem, SPLIT_KV)
    gq = [Gather(wq.at[j], wq_sem.at[j], SPLIT_Q) for j in range(2)]

    def add(buf, shard, at, first=False):
        width = 256

        @pl.loop(0, buf.shape[2] // width)
        def _(j):
            cols = tile(j, width)
            to = pl.ds(pl.multiple_of(at.start + j * width, width), width)
            part = jnp.dot(normed[shard], buf[shard, :, cols], preferred_element_type=jnp.float32)
            acc[:, to] = part if first else acc[:, to] + part

    def add_kv(*shards, first=False):
        for s in shards:
            add(wkv, s, pl.ds(0, 2 * nk), first)

    def add_q(j, *shards, first=False):
        for s in shards:
            add(wq.at[j], s, pl.ds(2 * nk + j * nk, nk), first)

    gkv.send(own, A, to_up, to_pair)
    gkv.send(own, B, to_down, to_cross)
    gkv.send(own, B, to_up)
    gkv.send(own, A, to_down)
    for dev in group:
        send(pos_ref, posb.at[ctx], pos_sem.at[ctx], dev)
    posb[ctx] = pos_ref[...]

    loads[2].wait()
    block = 64

    @pl.loop(0, rows // block)
    def _(i):
        at = tile(i, block)
        value = xv[at, :].astype(jnp.float32)
        scale = lax.rsqrt(jnp.mean(value * value, -1, keepdims=True) + 1e-06)
        out = (value * scale * gain_ref[...]).astype(jnp.bfloat16)
        for s in range(SHARDS):
            normed[s, at, :] = out[:, s * depth : (s + 1) * depth]

    for load in loads[3:]:
        load.wait()
    num[...] = jnp.zeros_like(num)
    add_kv(own, first=True)

    gkv.relay(down_own, A, to_up, to_pair, to_peer)
    gkv.relay(up_own, B, to_down, to_cross, to_peer)
    gkv.relay(pair, A, to_peer)
    gkv.relay(pair, B, to_peer)
    gkv.complete(pair)
    add_kv(pair)

    def start_z(g):
        g.send(own, A, to_up)
        g.send(own, B, to_down)
        g.send(own, B, to_up)
        g.send(own, A, to_down)

    def start_y(g):
        g.send(own, A, to_pair)
        g.send(own, B, to_cross)

    gkv.relay(down_own, B, to_cross, to_peer)
    gkv.relay(up_own, A, to_pair, to_peer)
    start_z(gq[0])
    gkv.relay(down_oth, A, to_peer)
    gkv.relay(up_oth, B, to_peer)
    gkv.complete(down_own, up_own)
    add_kv(down_own, up_own)

    gkv.relay(far_own, A, to_pair, to_peer)
    gkv.relay(far_own, B, to_cross, to_peer)
    start_y(gq[0])
    gkv.relay(up_oth, A, to_peer)
    gkv.relay(down_oth, B, to_peer)
    gkv.complete(down_oth, up_oth, far_own)
    add_kv(down_oth, up_oth, far_own)
    add_q(0, own, first=True)

    gq[0].relay(down_own, A, to_up, to_pair, to_peer)
    gq[0].relay(up_own, B, to_down, to_cross, to_peer)
    start_z(gq[1])
    gkv.relay(far_oth, A, to_peer)
    gkv.relay(far_oth, B, to_peer)
    gq[0].relay(down_own, B, to_cross, to_peer)
    gq[0].relay(up_own, A, to_pair, to_peer)
    gkv.complete(far_oth)
    add_kv(far_oth)

    def rope(u):
        return u * cos_ref[...] + pltpu.roll(u, hd // 2, 1) * sin_ref[...]

    for j in range(2):
        for ref, base in ((kvb.at[ctx], par * 2), (kvx, other * 2)):
            ref[j, :, :hd] = rope(acc[:, tile(base + j, hd)]).astype(jnp.bfloat16)
            ref[j, :, hd:] = acc[:, tile(nk // hd + base + j, hd)].astype(jnp.bfloat16)

    def kv_half(blk, j, half):
        return kvb.at[blk, j, pl.ds(half * half_rows, half_rows), :]

    def kv_send(blk, j, half, *devs):
        for dev in devs:
            ref = kv_half(blk, j, half)
            send(ref, ref, kv_sem.at[blk, j, half], dev)

    def kv_wait(blk, j, half):
        await_copy(kv_half(blk, j, half), kv_sem.at[blk, j, half])

    def kv_to_pair(j):
        for half in range(2):
            send(
                kvx.at[j, pl.ds(half * half_rows, half_rows), :], kv_half(ctx, j, half),
                kv_sem.at[ctx, j, half], to_pair,
            )

    def kv_to_z(blk, j):
        for half in range(2):
            kv_send(blk, j, half, to_up)
            kv_send(blk, j, 1 - half, to_down)

    def kv_relay(low, high, j):
        kv_wait(low, j, 0)
        kv_send(low, j, 0, to_up)
        kv_wait(high, j, 1)
        kv_send(high, j, 1, to_down)
        kv_wait(low, j, 1)
        kv_wait(high, j, 0)

    kv_to_pair(0)
    kv_to_z(ctx, 0)
    gq[0].relay(far_own, A, to_pair, to_peer)
    gq[0].relay(far_own, B, to_cross, to_peer)
    start_y(gq[1])
    gq[0].relay(pair, A, to_peer)
    gq[0].relay(pair, B, to_peer)
    gq[1].relay(down_own, A, to_up, to_pair, to_peer)
    gq[1].relay(up_own, B, to_down, to_cross, to_peer)
    gq[0].relay(down_oth, A, to_peer)
    gq[0].relay(up_oth, B, to_peer)
    gq[0].complete(pair, down_own, up_own)
    add_q(0, pair, down_own, up_own)
    gq[1].relay(down_own, B, to_cross, to_peer)
    gq[1].relay(up_own, A, to_pair, to_peer)
    gq[0].relay(up_oth, A, to_peer)
    gq[0].relay(down_oth, B, to_peer)
    kv_wait(pair, 0, 0)
    kv_wait(pair, 0, 1)
    kv_to_z(pair, 0)
    kv_to_pair(1)
    gq[0].complete(down_oth, up_oth, far_own)
    add_q(0, down_oth, up_oth, far_own)
    kv_relay(down_own, up_own, 0)
    kv_to_z(ctx, 1)
    gq[0].relay(far_oth, A, to_peer)
    gq[0].relay(far_oth, B, to_peer)
    gq[0].complete(far_oth)
    add_q(0, far_oth)

    def query(j):
        for r in range(2):
            at = slice(r * rows, (r + 1) * rows)
            for ref, base in ((qx, other), (qb.at[0], par)):
                u = acc[:, tile(2 * nk // hd + j * (nk // hd) + base * 2 + r, hd)]
                ref[j, at, :] = (rope(u) * query_scale).astype(jnp.bfloat16)
        send(qx.at[j], qb.at[1, j], q_sem.at[j], to_pair)

    query(0)
    gq[1].relay(far_own, A, to_pair, to_peer)
    gq[1].relay(far_own, B, to_cross, to_peer)

    for i in range(1, SHARDS):
        blk = (ctx + SHARDS - i) % SHARDS
        await_copy(posb.at[blk], pos_sem.at[blk])
    for src, blk in ((0, ctx), (1, pair)):
        col = jnp.transpose(posb[blk])[:, :1]
        for r in range(2):
            qpos[src, r * rows : (r + 1) * rows, :] = col

    def unit(src, j, step):
        zr = (z + step + step // 2 - 2 * (step // 3)) % 4
        blocks = pl.ds(zr * 2, 2)
        kk = kvb[blocks, j, :, :hd].reshape(2 * rows, hd)
        vv = kvb[blocks, j, :, hd:].reshape(2 * rows, hd)
        vv = jnp.concatenate([vv, jnp.ones_like(vv)], 1)
        kp = jnp.concatenate([posb[zr * 2, :1, :], posb[zr * 2 + 1, :1, :]], 1)
        s = lax.dot_general(
            qb[src, j], kk, (((1,), (1,)), ((), ())), preferred_element_type=jnp.float32
        )
        w = jnp.exp2(jnp.tanh(s * 0.02) * EXP_SCALE)
        w = jnp.where(kp <= qpos[src], w, 0.0).astype(jnp.bfloat16)
        num[src, j] += jnp.dot(w, vv, preferred_element_type=jnp.float32)

    def units(src, j, first, last):
        if last - first == 1:
            unit(src, j, first)
        else:
            pl.loop(first, last)(lambda i: unit(src, j, i))

    def result(src, j, r):
        n = num[src, j, r * rows : (r + 1) * rows, :]
        return (n[:, :hd] / n[:, hd:]).astype(jnp.bfloat16)

    def give_back(j):
        for r in range(2):
            osend[2 * j + r] = result(1, j, r)
            send(osend.at[2 * j + r], orecv.at[2 * j + r], o_sem.at[2 * j + r], to_pair)

    def far_wait(j):
        for blk in (far_own, far_oth):
            kv_wait(blk, j, 0)
            kv_wait(blk, j, 1)

    units(0, 0, 0, 1)
    gq[1].relay(pair, A, to_peer)
    gq[1].relay(pair, B, to_peer)
    gq[1].relay(down_oth, A, to_peer)
    gq[1].relay(up_oth, B, to_peer)
    kv_relay(down_oth, up_oth, 0)
    units(0, 0, 1, 3)
    add_q(1, own, first=True)
    gq[1].complete(pair, down_own, up_own)
    add_q(1, pair, down_own, up_own)
    gq[1].relay(up_oth, A, to_peer)
    gq[1].relay(down_oth, B, to_peer)
    kv_wait(pair, 1, 0)
    kv_wait(pair, 1, 1)
    kv_to_z(pair, 1)
    gq[1].complete(down_oth, up_oth, far_own)
    add_q(1, down_oth, up_oth, far_own)
    await_copy(qb.at[1, 0], q_sem.at[0])
    units(1, 0, 0, 3)
    gq[1].relay(far_oth, A, to_peer)
    gq[1].relay(far_oth, B, to_peer)
    gq[1].complete(far_oth)
    add_q(1, far_oth)
    query(1)
    far_wait(0)
    units(1, 0, 3, 4)
    give_back(0)
    kv_relay(down_own, up_own, 1)
    units(0, 0, 3, 4)
    units(0, 1, 0, 1)
    kv_relay(down_oth, up_oth, 1)
    units(0, 1, 1, 3)
    await_copy(qb.at[1, 1], q_sem.at[1])
    units(1, 1, 0, 3)
    far_wait(1)
    units(1, 1, 3, 4)
    give_back(1)
    units(0, 1, 3, 4)

    for j in range(2):
        for r in range(2):
            o_ref[:, tile(par * 4 + 2 * j + r, hd)] = result(0, j, r)
    for h in range(4):
        await_copy(orecv.at[h], o_sem.at[h])
        o_ref[:, tile(other * 4 + h, hd)] = orecv[h]

    for copy in sends:
        copy.wait_send()


def on_device(tokens, token_pos, norm_gain, query_weight, key_weight, value_weight):
    rows, feats = tokens.shape
    depth, nq = query_weight.shape
    nk = key_weight.shape[1]
    half = HEAD_DIM // 2
    freq = 10000.0 ** (-jnp.arange(half, dtype=jnp.float32) * 2.0 / HEAD_DIM)
    position = token_pos.astype(jnp.float32)
    angle = position[:, None] * freq[None, :]
    cosine, sine = jnp.cos(angle), jnp.sin(angle)
    cosine = jnp.concatenate([cosine, cosine], -1)
    sine = jnp.concatenate([-sine, sine], -1)
    vmem = pl.BlockSpec(memory_space=pltpu.VMEM)
    hbm = pl.BlockSpec(memory_space=pl.ANY)
    bf16, f32 = jnp.bfloat16, jnp.float32
    dma = pltpu.SemaphoreType.DMA
    return pl.pallas_call(
        kernel,
        out_shape=jax.ShapeDtypeStruct((rows, nq), bf16),
        in_specs=[hbm, vmem, hbm, hbm, hbm, vmem, vmem, vmem],
        out_specs=vmem,
        scratch_shapes=[
            pltpu.VMEM((rows, feats), bf16),
            pltpu.VMEM((SHARDS, rows, depth), bf16),
            pltpu.VMEM((SHARDS, depth, 2 * nk), bf16),
            pltpu.VMEM((2, SHARDS, depth, nk), bf16),
            pltpu.VMEM((rows, nq + 2 * nk), f32),
            pltpu.VMEM((SHARDS, 8, rows), f32),
            pltpu.VMEM((2, 2 * rows, 1), f32),
            pltpu.VMEM((SHARDS, 2, rows, 2 * HEAD_DIM), bf16),
            pltpu.VMEM((2, rows, 2 * HEAD_DIM), bf16),
            pltpu.VMEM((2, 2, 2 * rows, HEAD_DIM), bf16),
            pltpu.VMEM((2, 2 * rows, HEAD_DIM), bf16),
            pltpu.VMEM((2, 2, 2 * rows, 2 * HEAD_DIM), f32),
            pltpu.VMEM((4, rows, HEAD_DIM), bf16),
            pltpu.VMEM((4, rows, HEAD_DIM), bf16),
            dma((7,)),
            dma((136,)),
            dma((SHARDS, 4)),
            dma((2, SHARDS, 4)),
            dma((SHARDS, 2, 2)),
            dma((2,)),
            dma((4,)),
            dma((SHARDS,)),
        ],
        compiler_params=pltpu.CompilerParams(
            collective_id=0, has_side_effects=True, vmem_limit_bytes=62 * 1024 * 1024
        ),
        name="block",
    )(
        tokens, norm_gain.reshape(1, feats), query_weight, key_weight, value_weight,
        cosine, sine, jnp.broadcast_to(position[None, :], (8, rows)),
    )


def solution(mesh):
    in_specs = (
        P(("grp", "ctx"), None),
        P(("grp", "ctx")),
        P(),
        P("ctx", "tp"),
        P("ctx", "tp"),
        P("ctx", "tp"),
    )
    out_specs = P(("grp", "ctx"), "tp")
    return jax.shard_map(
        on_device, mesh=mesh, in_specs=in_specs, out_specs=out_specs, check_vma=False
    )
```

```python
import functools
import math

import jax
import jax.numpy as jnp
import numpy as np
from jax import lax
from jax.experimental import pallas as pl
from jax.experimental.pallas import tpu as pltpu
from jax.sharding import PartitionSpec as P

HEAD_DIM = 128
MESH = pl.DeviceIdType.MESH
query_scale = 144.0 ** (-0.5)
EXP_SCALE = 50.0 * math.log2(math.e)
SHARDS = 8
SPLITS = (144, 128, 112, 128)


def tile(index, size):
    return pl.ds(pl.multiple_of(index * size, size), size)


def kernel(
    x_hbm, gain_ref, wq_hbm, wk_hbm, wv_hbm, freq_ref, pos_ref,
    o_ref,
    cos_ref, sin_ref, xv, normed, weights, acc, posb, qpos, kvb, kvx, qb, qx, num, osend, orecv,
    local_sem, send_sem, weight_sem, kv_sem, q_sem, o_sem, pos_sem,
):
    ctx = lax.axis_index("ctx")
    grp = lax.axis_index("grp")
    z, par = ctx // 2, ctx % 2
    y_hi, core = grp // 2, grp % 2
    up, down, far = (z + 1) % 4, (z + 3) % 4, (z + 2) % 4
    other = 1 - par
    pair = z * 2 + other
    to_up = {"ctx": up * 2 + par}
    to_down = {"ctx": down * 2 + par}
    to_pair = {"ctx": pair}
    to_cross = {"ctx": pair, "grp": (1 - y_hi) * 2 + core}
    to_peer = {"grp": y_hi * 2 + (1 - core)}
    group = [{"ctx": (ctx + i) % SHARDS} for i in range(1, SHARDS)]

    rows, feats = xv.shape
    depth = weights.shape[2]
    nq, nk = wq_hbm.shape[1], wk_hbm.shape[1]
    hd = HEAD_DIM
    half_rows = rows // 2

    barrier = pltpu.get_barrier_semaphore()
    for dev in group + [to_cross, to_peer]:
        pl.semaphore_signal(barrier, inc=1, device_id=dev, device_id_type=MESH)
    loads = []

    def load(src, dst):
        loads.append(pltpu.make_async_copy(src, dst, local_sem.at[len(loads)]))

    for j in range(2):
        for i in range(2):
            for at, ref in ((i, wk_hbm), (2 + i, wv_hbm)):
                load(
                    ref.at[:, pl.ds((2 * i + j) * hd, hd)],
                    weights.at[j, ctx, :, pl.ds(at * hd, hd)],
                )
    for j in range(2):
        for i in range(2):
            load(
                wq_hbm.at[:, pl.ds((2 * i + j) * 2 * hd, 2 * hd)],
                weights.at[2 + j, ctx, :, pl.ds(i * 2 * hd, 2 * hd)],
            )
    load(x_hbm, xv)
    for item in loads[:8] + loads[-1:] + loads[8:-1]:
        item.start()
    for item in loads[:4]:
        item.wait()
    pl.semaphore_wait(barrier, SHARDS + 1)

    sends = []

    def copy_of(src, dst, recv, dev, at):
        return pltpu.make_async_remote_copy(
            src_ref=src, dst_ref=dst, send_sem=send_sem.at[at], recv_sem=recv,
            device_id=dev, device_id_type=MESH,
        )

    def send(src, dst, recv, dev):
        copy = copy_of(src, dst, recv, dev, len(sends))
        copy.start()
        sends.append(copy)

    def await_copy(dst, recv):
        copy_of(dst, dst, recv, to_peer, 0).wait_recv()

    class Gather:
        def __init__(self, buf, sem, split):
            self.buf, self.sem, self.split = buf, sem, split

        def piece(self, shard, owner, kind):
            base = owner * (depth // 2) + (self.split if kind else 0)
            size = depth // 2 - self.split if kind else self.split
            return self.buf.at[shard, pl.ds(pl.multiple_of(base, 16), size), :]

        def send(self, shard, kind, *devs):
            ref = self.piece(shard, core, kind)
            for dev in devs:
                send(ref, ref, self.sem.at[shard, core * 2 + kind], dev)

        def wait(self, shard, kind, owner=core):
            await_copy(self.piece(shard, owner, kind), self.sem.at[shard, owner * 2 + kind])

        def relay(self, shard, kind, *devs):
            self.wait(shard, kind)
            self.send(shard, kind, *devs)

        def complete(self, *shards):
            for s in shards:
                self.wait(s, 0, 1 - core)
                self.wait(s, 1, 1 - core)

    A, B = 0, 1
    own = ctx
    up_own, up_oth = up * 2 + par, up * 2 + other
    down_own, down_oth = down * 2 + par, down * 2 + other
    far_own, far_oth = far * 2 + par, far * 2 + other

    g = [Gather(weights.at[p], weight_sem.at[p], SPLITS[p]) for p in range(4)]

    def add(p, *shards, first=False):
        width = 256

        @pl.loop(0, nk // width)
        def _(i):
            cols = tile(i, width)
            part = sum(
                jnp.dot(normed[s], weights[p, s, :, cols], preferred_element_type=jnp.float32)
                for s in shards
            )
            acc[p, :, cols] = part if first else acc[p, :, cols] + part

    def a1(p):
        g[p].relay(down_own, A, to_up, to_pair, to_peer)
        g[p].relay(up_own, B, to_down, to_cross, to_peer)

    def a2(p):
        g[p].relay(down_own, B, to_cross, to_peer)
        g[p].relay(up_own, A, to_pair, to_peer)

    def a3(p):
        g[p].relay(far_own, A, to_pair, to_peer)
        g[p].relay(far_own, B, to_cross, to_peer)

    def y0(p):
        g[p].relay(pair, A, to_peer)
        g[p].relay(pair, B, to_peer)

    def y1(p):
        g[p].relay(down_oth, A, to_peer)
        g[p].relay(up_oth, B, to_peer)

    def y2(p):
        g[p].relay(up_oth, A, to_peer)
        g[p].relay(down_oth, B, to_peer)

    def y3(p):
        g[p].relay(far_oth, A, to_peer)
        g[p].relay(far_oth, B, to_peer)

    def start_z(p):
        g[p].send(own, A, to_up)
        g[p].send(own, B, to_down)
        g[p].send(own, B, to_up)
        g[p].send(own, A, to_down)

    def start_y(p):
        g[p].send(own, A, to_pair)
        g[p].send(own, B, to_cross)

    def finish(p, *shards):
        g[p].complete(*shards)
        add(p, *shards)

    start_z(0)
    start_y(0)
    posb[ctx] = jnp.broadcast_to(pos_ref[...].reshape(1, rows), (8, rows)).astype(jnp.float32)
    for item in loads[4:8]:
        item.wait()
    start_y(1)

    loads[-1].wait()
    block = 64
    gain = gain_ref[...].reshape(1, feats)

    @pl.loop(0, rows // block)
    def _(i):
        at = tile(i, block)
        value = xv[at, :].astype(jnp.float32)
        scale = lax.rsqrt(jnp.mean(value * value, -1, keepdims=True) + 1e-06)
        out = (value * scale * gain).astype(jnp.bfloat16)
        for s in range(SHARDS):
            normed[s, at, :] = out[:, s * depth : (s + 1) * depth]

    for item in loads[8:-1]:
        item.wait()

    def angles():
        angle = jnp.transpose(posb[ctx])[:, :1] * freq_ref[...]
        k = jnp.floor(angle * (2.0 / math.pi) + 0.5)
        t = angle - k * 1.5703125
        t = t - k * 4.8375129699707031e-4
        t = t - k * 7.5497899548918822e-8
        q = k - 4.0 * jnp.floor(k * 0.25)
        s = t * t
        sin = t + t * s * (-1.6666654611e-1 + s * (8.3321608736e-3 - s * 1.9515295891e-4))
        cos = 1.0 - 0.5 * s + s * s * (
            4.166664568298827e-2 + s * (s * 2.443315711809948e-5 - 1.388731625493765e-3)
        )
        odd = (q == 1.0) | (q == 3.0)
        sine = jnp.where(odd, cos, sin)
        cosine = jnp.where(odd, sin, cos)
        lane = lax.broadcasted_iota(jnp.int32, sine.shape, 1)
        sin_ref[...] = jnp.where((q >= 2.0) ^ (lane < hd // 2), -sine, sine)
        cos_ref[...] = jnp.where((q == 1.0) | (q == 2.0), -cosine, cosine)

    def rope(u):
        return u * cos_ref[...] + pltpu.roll(u, hd // 2, 1) * sin_ref[...]

    def keys_values(j):
        for ref, base in ((kvb.at[ctx], par), (kvx, other)):
            ref[j, :, :hd] = rope(acc[j, :, tile(base, hd)]).astype(jnp.bfloat16)
            ref[j, :, hd:] = acc[j, :, tile(2 + base, hd)].astype(jnp.bfloat16)

    def query(j):
        for r in range(2):
            at = slice(r * rows, (r + 1) * rows)
            for ref, base in ((qx, other), (qb.at[0], par)):
                u = acc[2 + j, :, tile(base * 2 + r, hd)]
                ref[j, at, :] = (rope(u) * query_scale).astype(jnp.bfloat16)
            send(qx.at[j, at, :], qb.at[1, j, at, :], q_sem.at[j, r], to_pair)

    def query_wait(j, r):
        at = slice(r * rows, (r + 1) * rows)
        await_copy(qb.at[1, j, at, :], q_sem.at[j, r])

    def kv_half(blk, j, half):
        return kvb.at[blk, j, pl.ds(half * half_rows, half_rows), :]

    def kv_send(blk, j, half, *devs):
        for dev in devs:
            ref = kv_half(blk, j, half)
            send(ref, ref, kv_sem.at[blk, j, half], dev)

    def kv_wait(blk, j, half):
        await_copy(kv_half(blk, j, half), kv_sem.at[blk, j, half])

    def kv_to_pair(j):
        for half in range(2):
            send(
                kvx.at[j, pl.ds(half * half_rows, half_rows), :], kv_half(ctx, j, half),
                kv_sem.at[ctx, j, half], to_pair,
            )

    def kv_to_z(blk, j):
        for half in range(2):
            kv_send(blk, j, half, to_up)
            kv_send(blk, j, 1 - half, to_down)

    def kv_pair(j):
        kv_wait(pair, j, 0)
        kv_wait(pair, j, 1)
        kv_to_z(pair, j)

    def kv_relay(low, high, j):
        kv_wait(low, j, 0)
        kv_send(low, j, 0, to_up)
        kv_wait(high, j, 1)
        kv_send(high, j, 1, to_down)
        kv_wait(low, j, 1)
        kv_wait(high, j, 0)

    def unit(src, j, step, at=slice(None)):
        zr = (z + step + step // 2 - 2 * (step // 3)) % 4
        blocks = pl.ds(zr * 2, 2)
        kk = kvb[blocks, j, :, :hd].reshape(2 * rows, hd)
        vv = kvb[blocks, j, :, hd:].reshape(2 * rows, hd)
        vv = jnp.concatenate([vv, jnp.ones_like(vv)], 1)
        kp = jnp.concatenate([posb[zr * 2, :1, :], posb[zr * 2 + 1, :1, :]], 1)
        s = lax.dot_general(
            qb[src, j, at, :], kk, (((1,), (1,)), ((), ())), preferred_element_type=jnp.float32
        )
        w = jnp.exp2(jnp.tanh(s * 0.02) * EXP_SCALE)
        w = jnp.where(kp <= qpos[src, at, :], w, 0.0).astype(jnp.bfloat16)
        num[src, j, at, :] += jnp.dot(w, vv, preferred_element_type=jnp.float32)

    def units(src, j, first, last):
        if last - first == 1:
            unit(src, j, first)
        else:
            pl.loop(first, last)(lambda i: unit(src, j, i))

    halves = [slice(r * rows, (r + 1) * rows) for r in range(2)]

    def result(src, j, r):
        n = num[src, j, r * rows : (r + 1) * rows, :]
        return (n[:, :hd] / n[:, hd:]).astype(jnp.bfloat16)

    def give_back(j, r):
        osend[2 * j + r] = result(1, j, r)
        send(osend.at[2 * j + r], orecv.at[2 * j + r], o_sem.at[2 * j + r], to_pair)

    def far_wait(j):
        for blk in (far_own, far_oth):
            kv_wait(blk, j, 0)
            kv_wait(blk, j, 1)

    add(0, own, first=True)
    for dev in group:
        send(posb.at[ctx], posb.at[ctx], pos_sem.at[ctx], dev)
    angles()
    a1(0)
    start_z(1)
    y0(0)
    num[...] = jnp.zeros_like(num)
    a2(0)
    y0(1)
    finish(0, pair)
    a3(0)
    y1(0)
    finish(0, down_own, up_own)
    a1(1)
    start_z(2)
    y2(0)
    add(1, own, first=True)
    finish(1, pair)
    a2(1)
    y3(0)
    finish(0, down_oth, up_oth, far_own)
    finish(0, far_oth)
    keys_values(0)
    kv_to_pair(0)
    a3(1)
    y1(1)
    start_y(2)
    finish(1, down_own, up_own)
    a1(2)
    start_z(3)
    kv_to_z(ctx, 0)
    y2(1)
    add(2, own, first=True)
    a2(2)
    for i in range(1, SHARDS):
        blk = (ctx + SHARDS - i) % SHARDS
        await_copy(posb.at[blk], pos_sem.at[blk])
    for src, blk in ((0, ctx), (1, pair)):
        col = jnp.transpose(posb[blk])[:, :1]
        for r in range(2):
            qpos[src, r * rows : (r + 1) * rows, :] = col
    finish(1, down_oth, up_oth, far_own)
    a3(2)
    start_y(3)
    y3(1)
    finish(1, far_oth)
    keys_values(1)
    a1(3)
    kv_pair(0)
    y0(2)
    a2(3)
    y1(2)
    finish(2, pair, down_own, up_own)
    y2(2)
    kv_relay(down_own, up_own, 0)
    finish(2, down_oth, up_oth, far_own)
    y3(2)
    finish(2, far_oth)
    query(0)
    a3(3)
    units(0, 0, 0, 1)
    y0(3)
    y1(3)
    kv_to_pair(1)
    add(3, own, first=True)
    finish(3, pair, down_own, up_own)
    kv_relay(down_oth, up_oth, 0)
    kv_to_z(ctx, 1)
    y2(3)
    units(0, 0, 1, 3)
    query_wait(0, 0)
    query_wait(0, 1)
    units(1, 0, 0, 1)
    kv_pair(1)
    y3(3)
    finish(3, down_oth, up_oth, far_own)
    units(1, 0, 1, 2)
    finish(3, far_oth)
    query(1)
    units(1, 0, 2, 3)
    far_wait(0)
    units(1, 0, 3, 4)
    give_back(0, 0)
    give_back(0, 1)
    kv_relay(down_own, up_own, 1)
    units(0, 0, 3, 4)
    units(0, 1, 0, 1)
    kv_relay(down_oth, up_oth, 1)
    units(0, 1, 1, 3)
    for r in range(2):
        query_wait(1, r)
        unit(1, 1, 0, halves[r])
    units(1, 1, 1, 3)
    far_wait(1)
    for r in range(2):
        unit(1, 1, 3, halves[r])
        give_back(1, r)
    units(0, 1, 3, 4)

    for j in range(2):
        for r in range(2):
            o_ref[:, tile(par * 4 + 2 * j + r, hd)] = result(0, j, r)
    for h in range(4):
        await_copy(orecv.at[h], o_sem.at[h])
        o_ref[:, tile(other * 4 + h, hd)] = orecv[h]

    for copy in sends:
        copy.wait_send()


def on_device(tokens, token_pos, norm_gain, query_weight, key_weight, value_weight):
    rows, feats = tokens.shape
    depth, nq = query_weight.shape
    nk = key_weight.shape[1]
    half = HEAD_DIM // 2
    freq = (10000.0 ** (-np.arange(half) * 2.0 / HEAD_DIM)).astype(np.float32)
    freq = jnp.asarray(np.concatenate([freq, freq])[None, :])
    vmem = pl.BlockSpec(memory_space=pltpu.VMEM)
    hbm = pl.BlockSpec(memory_space=pl.ANY)
    bf16, f32 = jnp.bfloat16, jnp.float32
    dma = pltpu.SemaphoreType.DMA
    return pl.pallas_call(
        kernel,
        out_shape=jax.ShapeDtypeStruct((rows, nq), bf16),
        in_specs=[hbm, vmem, hbm, hbm, hbm, vmem, vmem],
        out_specs=vmem,
        scratch_shapes=[
            pltpu.VMEM((rows, HEAD_DIM), f32),
            pltpu.VMEM((rows, HEAD_DIM), f32),
            pltpu.VMEM((rows, feats), bf16),
            pltpu.VMEM((SHARDS, rows, depth), bf16),
            pltpu.VMEM((4, SHARDS, depth, nk), bf16),
            pltpu.VMEM((4, rows, nk), f32),
            pltpu.VMEM((SHARDS, 8, rows), f32),
            pltpu.VMEM((2, 2 * rows, 1), f32),
            pltpu.VMEM((SHARDS, 2, rows, 2 * HEAD_DIM), bf16),
            pltpu.VMEM((2, rows, 2 * HEAD_DIM), bf16),
            pltpu.VMEM((2, 2, 2 * rows, HEAD_DIM), bf16),
            pltpu.VMEM((2, 2 * rows, HEAD_DIM), bf16),
            pltpu.VMEM((2, 2, 2 * rows, 2 * HEAD_DIM), f32),
            pltpu.VMEM((4, rows, HEAD_DIM), bf16),
            pltpu.VMEM((4, rows, HEAD_DIM), bf16),
            dma((13,)),
            dma((160,)),
            dma((4, SHARDS, 4)),
            dma((SHARDS, 2, 2)),
            dma((2, 2)),
            dma((4,)),
            dma((SHARDS,)),
        ],
        compiler_params=pltpu.CompilerParams(
            collective_id=0, has_side_effects=True, vmem_limit_bytes=62 * 1024 * 1024
        ),
        name="block",
    )(
        tokens, norm_gain, query_weight, key_weight, value_weight, freq, token_pos,
    )


def solution(mesh):
    in_specs = (
        P(("grp", "ctx"), None),
        P(("grp", "ctx")),
        P(),
        P("ctx", "tp"),
        P("ctx", "tp"),
        P("ctx", "tp"),
    )
    out_specs = P(("grp", "ctx"), "tp")
    return jax.shard_map(
        on_device, mesh=mesh, in_specs=in_specs, out_specs=out_specs, check_vma=False
    )
```

```python
import functools
import math

import jax
import jax.numpy as jnp
import numpy as np
from jax import lax
from jax.experimental import pallas as pl
from jax.experimental.pallas import tpu as pltpu
from jax.sharding import PartitionSpec as P

HEAD_DIM = 128
MESH = pl.DeviceIdType.MESH
query_scale = 144.0 ** (-0.5)
EXP_SCALE = 50.0 * math.log2(math.e)
SHARDS = 8
SENDS = 32
SPLITS = (144, 128, 112, 128)


def tile(index, size):
    return pl.ds(pl.multiple_of(index * size, size), size)


def kernel(
    x_hbm, gain_hbm, wq_hbm, wk_hbm, wv_hbm, freq_hbm, pos_hbm,
    o_hbm,
    gain_ref, freq_ref, pos_ref, cos_ref, sin_ref, xv, normed, weights, acc, posb, qpos, kvb, kvx, qb, qx, num, oown, osend,
    local_sem, out_sem, send_sem, weight_sem, kv_sem, q_sem, o_sem, pos_sem,
):
    ctx = lax.axis_index("ctx")
    grp = lax.axis_index("grp")
    z, par = ctx // 2, ctx % 2
    y_hi, core = grp // 2, grp % 2
    up, down, far = (z + 1) % 4, (z + 3) % 4, (z + 2) % 4
    other = 1 - par
    pair = z * 2 + other
    to_up = {"ctx": up * 2 + par}
    to_down = {"ctx": down * 2 + par}
    to_pair = {"ctx": pair}
    to_cross = {"ctx": pair, "grp": (1 - y_hi) * 2 + core}
    to_peer = {"grp": y_hi * 2 + (1 - core)}
    group = [{"ctx": (ctx + i) % SHARDS} for i in range(1, SHARDS)]

    rows, feats = xv.shape
    depth = weights.shape[2]
    nq, nk = wq_hbm.shape[1], wk_hbm.shape[1]
    hd = HEAD_DIM
    half_rows = rows // 2

    barrier = pltpu.get_barrier_semaphore()
    for dev in group + [to_cross, to_peer]:
        pl.semaphore_signal(barrier, inc=1, device_id=dev, device_id_type=MESH)
    def load(src, dst, at):
        pltpu.make_async_copy(src, dst, local_sem.at[at]).start()

    def loaded(dst, at):
        pltpu.make_async_copy(dst, dst, local_sem.at[at]).wait()

    def load_kv(j):
        for i in range(2):
            for at, ref in ((i, wk_hbm), (2 + i, wv_hbm)):
                load(
                    ref.at[:, pl.ds((2 * i + j) * hd, hd)],
                    weights.at[j, ctx, :, pl.ds(at * hd, hd)],
                    j,
                )

    load_kv(0)
    load(x_hbm, xv, 4)
    load(gain_hbm, gain_ref, 5)
    load(pos_hbm, pos_ref, 6)
    load(freq_hbm, freq_ref, 7)
    load_kv(1)
    for j in range(2):
        for i in range(2):
            load(
                wq_hbm.at[:, pl.ds((2 * i + j) * 2 * hd, 2 * hd)],
                weights.at[2 + j, ctx, :, pl.ds(i * 2 * hd, 2 * hd)],
                2 + j,
            )
    loaded(weights.at[0, ctx], 0)
    pl.semaphore_wait(barrier, SHARDS + 1)

    sends = []

    def copy_of(src, dst, recv, dev, at):
        return pltpu.make_async_remote_copy(
            src_ref=src, dst_ref=dst, send_sem=send_sem.at[at % SENDS], recv_sem=recv,
            device_id=dev, device_id_type=MESH,
        )

    def send(src, dst, recv, dev):
        if len(sends) >= SENDS:
            sends[-SENDS].wait_send()
        copy = copy_of(src, dst, recv, dev, len(sends))
        copy.start()
        sends.append(copy)

    def await_copy(dst, recv):
        copy_of(dst, dst, recv, to_peer, 0).wait_recv()

    A, B = 0, 1
    own = ctx
    up_own, up_oth = up * 2 + par, up * 2 + other
    down_own, down_oth = down * 2 + par, down * 2 + other
    far_own, far_oth = far * 2 + par, far * 2 + other

    def add(p, *shards, first=False):
        width = 256

        @pl.loop(0, nk // width)
        def _(i):
            cols = tile(i, width)
            part = sum(
                jnp.dot(normed[s], weights[p, s, :, cols], preferred_element_type=jnp.float32)
                for s in shards
            )
            acc[p, :, cols] = part if first else acc[p, :, cols] + part

    DN, UP, FAR, PAIR, DNO, UPO, FARO, PEER = 0, 2, 4, 5, 6, 7, 8, 9
    peer_role = [(down_own, 0), (up_own, 1), (far_own, 2), (pair, 3)]
    peer_role += [(down_oth, 4), (up_oth, 5), (far_oth, 6)]

    def part(p, shard, kind):
        base = core * (depth // 2) + (SPLITS[p] if kind else 0)
        size = depth // 2 - SPLITS[p] if kind else SPLITS[p]
        return weights.at[p, shard, pl.ds(pl.multiple_of(base, 16), size), :]

    def side(p, shard, owner):
        return weights.at[p, shard, pl.ds(pl.multiple_of(owner * (depth // 2), 16), depth // 2), :]

    def send_part(p, shard, kind, role, dev):
        ref = part(p, shard, kind)
        send(ref, ref, weight_sem.at[p, role], dev)

    def to_other_core(p, at):
        shard, role = peer_role[at]
        ref = side(p, shard, core)
        send(ref, ref, weight_sem.at[p, PEER + role], to_peer)

    def wait_part(p, shard, kind, role):
        await_copy(part(p, shard, kind), weight_sem.at[p, role])

    def wait_side(p, shard, role):
        await_copy(side(p, shard, core), weight_sem.at[p, role])

    def a1(p):
        wait_part(p, down_own, A, DN + A)
        send_part(p, down_own, A, FAR, to_up)
        send_part(p, down_own, A, DNO, to_pair)
        wait_part(p, up_own, B, UP + B)
        send_part(p, up_own, B, FAR, to_down)
        send_part(p, up_own, B, UPO, to_cross)

    def a2(p):
        wait_part(p, down_own, B, DN + B)
        send_part(p, down_own, B, DNO, to_cross)
        to_other_core(p, 0)
        wait_part(p, up_own, A, UP + A)
        send_part(p, up_own, A, UPO, to_pair)
        to_other_core(p, 1)

    def a3(p):
        wait_side(p, far_own, FAR)
        send_part(p, far_own, A, FARO, to_pair)
        send_part(p, far_own, B, FARO, to_cross)
        to_other_core(p, 2)

    def y0(p):
        wait_side(p, pair, PAIR)
        to_other_core(p, 3)

    def y2(p):
        wait_side(p, down_oth, DNO)
        to_other_core(p, 4)
        wait_side(p, up_oth, UPO)
        to_other_core(p, 5)

    def y3(p):
        wait_side(p, far_oth, FARO)
        to_other_core(p, 6)

    def start_z(p):
        send_part(p, own, A, DN + A, to_up)
        send_part(p, own, B, UP + B, to_down)
        send_part(p, own, B, DN + B, to_up)
        send_part(p, own, A, UP + A, to_down)

    def start_y(p):
        send_part(p, own, A, PAIR, to_pair)
        send_part(p, own, B, PAIR, to_cross)

    def finish(p, *at):
        for i in at:
            shard, role = peer_role[i]
            await_copy(side(p, shard, 1 - core), weight_sem.at[p, PEER + role])
        add(p, *[peer_role[i][0] for i in at])

    dn_, up_, far_, pair_, dno_, upo_, faro_ = range(7)

    start_z(0)
    start_y(0)
    loaded(pos_ref, 6)
    posb[ctx] = jnp.broadcast_to(pos_ref[...].reshape(1, rows), (8, rows)).astype(jnp.float32)
    loaded(weights.at[1, ctx], 1)
    start_y(1)

    loaded(xv, 4)
    loaded(gain_ref, 5)
    loaded(freq_ref, 7)
    block = 64
    gain = gain_ref[...].reshape(1, feats)

    @pl.loop(0, rows // block)
    def _(i):
        at = tile(i, block)
        value = xv[at, :].astype(jnp.float32)
        scale = lax.rsqrt(jnp.mean(value * value, -1, keepdims=True) + 1e-06)
        out = (value * scale * gain).astype(jnp.bfloat16)
        for s in range(SHARDS):
            normed[s, at, :] = out[:, s * depth : (s + 1) * depth]

    loaded(weights.at[2, ctx], 2)
    loaded(weights.at[3, ctx], 3)

    def angles():
        angle = jnp.transpose(posb[ctx])[:, :1] * freq_ref[...]
        k = jnp.floor(angle * (2.0 / math.pi) + 0.5)
        t = angle - k * 1.5703125
        t = t - k * 4.8375129699707031e-4
        t = t - k * 7.5497899548918822e-8
        q = k - 4.0 * jnp.floor(k * 0.25)
        s = t * t
        sin = t + t * s * (-1.6666654611e-1 + s * (8.3321608736e-3 - s * 1.9515295891e-4))
        cos = 1.0 - 0.5 * s + s * s * (
            4.166664568298827e-2 + s * (s * 2.443315711809948e-5 - 1.388731625493765e-3)
        )
        odd = (q == 1.0) | (q == 3.0)
        sine = jnp.where(odd, cos, sin)
        cosine = jnp.where(odd, sin, cos)
        lane = lax.broadcasted_iota(jnp.int32, sine.shape, 1)
        sin_ref[...] = jnp.where((q >= 2.0) ^ (lane < hd // 2), -sine, sine)
        cos_ref[...] = jnp.where((q == 1.0) | (q == 2.0), -cosine, cosine)

    def rope(u):
        return u * cos_ref[...] + pltpu.roll(u, hd // 2, 1) * sin_ref[...]

    def keys_values(j):
        for ref, base in ((kvb.at[ctx], par), (kvx, other)):
            ref[j, :, :hd] = rope(acc[j, :, tile(base, hd)]).astype(jnp.bfloat16)
            ref[j, :, hd:] = acc[j, :, tile(2 + base, hd)].astype(jnp.bfloat16)

    def query(j):
        for r in range(2):
            at = slice(r * rows, (r + 1) * rows)
            for ref, base in ((qx, other), (qb.at[0], par)):
                u = acc[2 + j, :, tile(base * 2 + r, hd)]
                ref[j, at, :] = (rope(u) * query_scale).astype(jnp.bfloat16)
            send(qx.at[j, at, :], qb.at[1, j, at, :], q_sem.at[j, r], to_pair)

    def query_wait(j, r):
        at = slice(r * rows, (r + 1) * rows)
        await_copy(qb.at[1, j, at, :], q_sem.at[j, r])

    def kv_half(blk, j, half):
        return kvb.at[blk, j, pl.ds(half * half_rows, half_rows), :]

    def kv_send(blk, j, half, role, dev):
        ref = kv_half(blk, j, half)
        send(ref, ref, kv_sem.at[j, role], dev)

    def kv_to_pair(j):
        send(kvx.at[j], kvb.at[ctx, j], kv_sem.at[j, 0], to_pair)

    def kv_to_z(blk, j, base):
        for half in range(2):
            kv_send(blk, j, half, base + half, to_up)
            kv_send(blk, j, 1 - half, base + 2 + 1 - half, to_down)

    def kv_pair(j):
        await_copy(kvb.at[pair, j], kv_sem.at[j, 0])
        kv_to_z(pair, j, 6)

    def kv_relay(low, high, j, base):
        await_copy(kv_half(low, j, 0), kv_sem.at[j, base])
        kv_send(low, j, 0, base + 4, to_up)
        await_copy(kv_half(high, j, 1), kv_sem.at[j, base + 3])
        kv_send(high, j, 1, base + 4, to_down)
        await_copy(kv_half(low, j, 1), kv_sem.at[j, base + 1])
        await_copy(kv_half(high, j, 0), kv_sem.at[j, base + 2])

    def unit(src, j, step, at=slice(None)):
        zr = (z + step + step // 2 - 2 * (step // 3)) % 4
        blocks = pl.ds(zr * 2, 2)
        kk = kvb[blocks, j, :, :hd].reshape(2 * rows, hd)
        vv = kvb[blocks, j, :, hd:].reshape(2 * rows, hd)
        vv = jnp.concatenate([vv, jnp.ones_like(vv)], 1)
        kp = jnp.concatenate([posb[zr * 2, :1, :], posb[zr * 2 + 1, :1, :]], 1)
        s = lax.dot_general(
            qb[src, j, at, :], kk, (((1,), (1,)), ((), ())), preferred_element_type=jnp.float32
        )
        w = jnp.exp2(jnp.tanh(s * 0.02) * EXP_SCALE)
        w = jnp.where(kp <= qpos[src, at, :], w, 0.0).astype(jnp.bfloat16)
        num[src, j, at, :] += jnp.dot(w, vv, preferred_element_type=jnp.float32)

    def units(src, j, first, last):
        if last - first == 1:
            unit(src, j, first)
        else:
            pl.loop(first, last)(lambda i: unit(src, j, i))

    halves = [slice(r * rows, (r + 1) * rows) for r in range(2)]

    def result(src, j, r):
        n = num[src, j, r * rows : (r + 1) * rows, :]
        return (n[:, :hd] / n[:, hd:]).astype(jnp.bfloat16)

    def columns(base, h):
        return o_hbm.at[:, tile(base * 4 + h, hd)]

    def give_back(j, r):
        h = 2 * j + r
        osend[h] = result(1, j, r)
        send(osend.at[h], columns(par, h), o_sem.at[0], to_pair)

    def keep(j, r):
        h = 2 * j + r
        oown[h] = result(0, j, r)
        pltpu.make_async_copy(oown.at[h], columns(par, h), out_sem.at[0]).start()

    def far_wait(j):
        await_copy(kvb.at[far_own, j], kv_sem.at[j, 5])
        await_copy(kvb.at[far_oth, j], kv_sem.at[j, 10])

    add(0, own, first=True)
    for dev in group:
        send(posb.at[ctx], posb.at[ctx], pos_sem.at[0], dev)
    angles()
    a1(0)
    start_z(1)
    y0(0)
    num[...] = jnp.zeros_like(num)
    a2(0)
    y0(1)
    finish(0, pair_)
    a3(0)
    finish(0, dn_, up_)
    a1(1)
    start_z(2)
    y2(0)
    add(1, own, first=True)
    finish(1, pair_)
    a2(1)
    y3(0)
    finish(0, dno_, upo_, far_)
    finish(0, faro_)
    keys_values(0)
    kv_to_pair(0)
    a3(1)
    start_y(2)
    finish(1, dn_, up_)
    a1(2)
    start_z(3)
    kv_to_z(ctx, 0, 1)
    y2(1)
    add(2, own, first=True)
    a2(2)
    await_copy(posb.at[pl.ds(0, SHARDS - 1)], pos_sem.at[0])
    for src, blk in ((0, ctx), (1, pair)):
        col = jnp.transpose(posb[blk])[:, :1]
        for r in range(2):
            qpos[src, r * rows : (r + 1) * rows, :] = col
    finish(1, dno_, upo_, far_)
    a3(2)
    start_y(3)
    y3(1)
    finish(1, faro_)
    keys_values(1)
    a1(3)
    kv_pair(0)
    y0(2)
    a2(3)
    finish(2, pair_, dn_, up_)
    y2(2)
    kv_relay(down_own, up_own, 0, 1)
    finish(2, dno_, upo_, far_)
    y3(2)
    finish(2, faro_)
    query(0)
    a3(3)
    units(0, 0, 0, 1)
    y0(3)
    kv_to_pair(1)
    add(3, own, first=True)
    finish(3, pair_, dn_, up_)
    kv_relay(down_oth, up_oth, 0, 6)
    kv_to_z(ctx, 1, 1)
    y2(3)
    units(0, 0, 1, 3)
    query_wait(0, 0)
    query_wait(0, 1)
    units(1, 0, 0, 1)
    y3(3)
    finish(3, dno_, upo_, far_)
    kv_pair(1)
    units(1, 0, 1, 2)
    finish(3, faro_)
    query(1)
    units(1, 0, 2, 3)
    far_wait(0)
    units(1, 0, 3, 4)
    give_back(0, 0)
    give_back(0, 1)
    kv_relay(down_own, up_own, 1, 1)
    units(0, 0, 3, 4)
    keep(0, 0)
    keep(0, 1)
    units(0, 1, 0, 1)
    kv_relay(down_oth, up_oth, 1, 6)
    units(0, 1, 1, 3)
    for r in range(2):
        query_wait(1, r)
        unit(1, 1, 0, halves[r])
    units(1, 1, 1, 3)
    far_wait(1)
    for r in range(2):
        unit(1, 1, 3, halves[r])
        give_back(1, r)
    for r in range(2):
        unit(0, 1, 3, halves[r])
        keep(1, r)
    mine = o_hbm.at[:, tile(par, 4 * hd)]
    pltpu.make_async_copy(mine, mine, out_sem.at[0]).wait()
    await_copy(o_hbm.at[:, tile(other, 4 * hd)], o_sem.at[0])
    for copy in sends[-SENDS:]:
        copy.wait_send()


def on_device(tokens, token_pos, norm_gain, query_weight, key_weight, value_weight):
    rows, feats = tokens.shape
    depth, nq = query_weight.shape
    nk = key_weight.shape[1]
    half = HEAD_DIM // 2
    freq = (10000.0 ** (-np.arange(half) * 2.0 / HEAD_DIM)).astype(np.float32)
    freq = jnp.asarray(np.concatenate([freq, freq])[None, :])
    hbm = pl.BlockSpec(memory_space=pl.ANY)
    bf16, f32 = jnp.bfloat16, jnp.float32
    dma = pltpu.SemaphoreType.DMA
    return pl.pallas_call(
        kernel,
        out_shape=jax.ShapeDtypeStruct((rows, nq), bf16),
        in_specs=[hbm] * 7,
        out_specs=hbm,
        scratch_shapes=[
            pltpu.VMEM((feats,), f32),
            pltpu.VMEM((1, HEAD_DIM), f32),
            pltpu.VMEM((rows,), jnp.int32),
            pltpu.VMEM((rows, HEAD_DIM), f32),
            pltpu.VMEM((rows, HEAD_DIM), f32),
            pltpu.VMEM((rows, feats), bf16),
            pltpu.VMEM((SHARDS, rows, depth), bf16),
            pltpu.VMEM((4, SHARDS, depth, nk), bf16),
            pltpu.VMEM((4, rows, nk), f32),
            pltpu.VMEM((SHARDS, 8, rows), f32),
            pltpu.VMEM((2, 2 * rows, 1), f32),
            pltpu.VMEM((SHARDS, 2, rows, 2 * HEAD_DIM), bf16),
            pltpu.VMEM((2, rows, 2 * HEAD_DIM), bf16),
            pltpu.VMEM((2, 2, 2 * rows, HEAD_DIM), bf16),
            pltpu.VMEM((2, 2 * rows, HEAD_DIM), bf16),
            pltpu.VMEM((2, 2, 2 * rows, 2 * HEAD_DIM), f32),
            pltpu.VMEM((4, rows, HEAD_DIM), bf16),
            pltpu.VMEM((4, rows, HEAD_DIM), bf16),
            dma((8,)),
            dma((1,)),
            dma((SENDS,)),
            dma((4, 16)),
            dma((2, 11)),
            dma((2, 2)),
            dma((1,)),
            dma((1,)),
        ],
        compiler_params=pltpu.CompilerParams(
            collective_id=0, has_side_effects=True, vmem_limit_bytes=62 * 1024 * 1024
        ),
        name="block",
    )(
        tokens, norm_gain, query_weight, key_weight, value_weight, freq, token_pos,
    )


def solution(mesh):
    in_specs = (
        P(("grp", "ctx"), None),
        P(("grp", "ctx")),
        P(),
        P("ctx", "tp"),
        P("ctx", "tp"),
        P("ctx", "tp"),
    )
    out_specs = P(("grp", "ctx"), "tp")
    return jax.shard_map(
        on_device, mesh=mesh, in_specs=in_specs, out_specs=out_specs, check_vma=False
    )
```

```python
import functools
import math

import jax
import jax.numpy as jnp
import numpy as np
from jax import lax
from jax.experimental import pallas as pl
from jax.experimental.pallas import tpu as pltpu
from jax.sharding import PartitionSpec as P

HEAD_DIM = 128
MESH = pl.DeviceIdType.MESH
query_scale = 144.0 ** (-0.5)
EXP_SCALE = 50.0 * math.log2(math.e)
SHARDS = 8
SENDS = 64
SPLITS = (128, 112, 112, 112, 112)


def tile(index, size):
    return pl.ds(pl.multiple_of(index * size, size), size)


def kernel(
    x_hbm, gain_hbm, wq_hbm, wk_hbm, wv_hbm, freq_hbm, pos_hbm,
    o_hbm,
    gain_ref, freq_ref, pos_ref, cos_ref, sin_ref, xv, normed, weights, acc, posb, qpos, kvb, kvx, qb, qx, num, oown, osend,
    local_sem, out_sem, send_sem, weight_sem, kv_sem, q_sem, o_sem, pos_sem,
):
    ctx = lax.axis_index("ctx")
    grp = lax.axis_index("grp")
    z, par = ctx // 2, ctx % 2
    y_hi, core = grp // 2, grp % 2
    up, down, far = (z + 1) % 4, (z + 3) % 4, (z + 2) % 4
    other = 1 - par
    pair = z * 2 + other
    to_up = {"ctx": up * 2 + par}
    to_down = {"ctx": down * 2 + par}
    to_pair = {"ctx": pair}
    to_cross = {"ctx": pair, "grp": (1 - y_hi) * 2 + core}
    to_peer = {"grp": y_hi * 2 + (1 - core)}
    group = [{"ctx": (ctx + i) % SHARDS} for i in range(1, SHARDS)]

    rows, feats = xv.shape
    depth = weights.shape[2]
    nq, nk = wq_hbm.shape[1], wk_hbm.shape[1]
    hd = HEAD_DIM
    half_rows = rows // 2

    barrier = pltpu.get_barrier_semaphore()
    for dev in group + [to_cross, to_peer]:
        pl.semaphore_signal(barrier, inc=1, device_id=dev, device_id_type=MESH)
    def load(src, dst, at):
        pltpu.make_async_copy(src, dst, local_sem.at[at]).start()

    def loaded(dst, at):
        pltpu.make_async_copy(dst, dst, local_sem.at[at]).wait()

    def load_kv(j):
        for i in range(2):
            for at, ref in ((i, wk_hbm), (2 + i, wv_hbm)):
                load(
                    ref.at[:, pl.ds((2 * i + j) * hd, hd)],
                    weights.at[j, ctx, :, pl.ds(at * hd, hd)],
                    j,
                )

    def load_q(j):
        for r in range(2):
            for i in range(2):
                load(
                    wq_hbm.at[:, pl.ds((4 * i + 2 * j + r) * hd, hd)],
                    weights.at[2 + j, ctx, :, pl.ds((2 * r + i) * hd, hd)],
                    2 + j,
                )

    load_kv(0)
    load(x_hbm, xv, 4)
    load(gain_hbm, gain_ref, 5)
    load(pos_hbm, pos_ref, 6)
    load(freq_hbm, freq_ref, 7)
    load_q(0)
    load_kv(1)
    load_q(1)
    loaded(weights.at[0, ctx], 0)
    pl.semaphore_wait(barrier, SHARDS + 1)

    sends = []

    def copy_of(src, dst, recv, dev, at):
        return pltpu.make_async_remote_copy(
            src_ref=src, dst_ref=dst, send_sem=send_sem.at[at % SENDS], recv_sem=recv,
            device_id=dev, device_id_type=MESH,
        )

    def sent(at):
        count, width = sends[at]
        ref = weights.at[0, 0, pl.ds(0, count), pl.ds(0, width)]
        copy_of(ref, ref, weight_sem.at[0, 0], to_peer, at).wait_send()

    def send(src, dst, recv, dev):
        if len(sends) >= SENDS:
            sent(len(sends) - SENDS)
        copy_of(src, dst, recv, dev, len(sends)).start()
        count, width = src.shape[-2:]
        sends.append((count * src.dtype.itemsize // 2, width))

    def await_copy(dst, recv):
        copy_of(dst, dst, recv, to_peer, 0).wait_recv()

    A, B = 0, 1
    own = ctx
    up_own, up_oth = up * 2 + par, up * 2 + other
    down_own, down_oth = down * 2 + par, down * 2 + other
    far_own, far_oth = far * 2 + par, far * 2 + other

    places = [(0, 0, nk), (2, 0, nk), (1, 0, nk), (3, 0, nk // 2), (3, nk // 2, nk // 2)]

    def add(p, *shards, first=False):
        buf, start, count = places[p]
        width = 256

        @pl.loop(0, count // width)
        def _(i):
            cols = pl.ds(pl.multiple_of(start + i * width, width), width)
            part = sum(
                jnp.dot(normed[s], weights[buf, s, :, cols], preferred_element_type=jnp.float32)
                for s in shards
            )
            acc[buf, :, cols] = part if first else acc[buf, :, cols] + part

    DN, UP, FAR, PAIR, DNO, UPO, FARO, PEER = 0, 2, 4, 5, 6, 7, 8, 9
    peer_role = [(down_own, 0), (up_own, 1), (far_own, 2), (pair, 3)]
    peer_role += [(down_oth, 4), (up_oth, 5), (far_oth, 6)]

    def part(p, shard, kind):
        base = core * (depth // 2) + (SPLITS[p] if kind else 0)
        size = depth // 2 - SPLITS[p] if kind else SPLITS[p]
        buf, start, count = places[p]
        return weights.at[buf, shard, pl.ds(pl.multiple_of(base, 16), size), pl.ds(start, count)]

    def side(p, shard, owner):
        at = pl.ds(pl.multiple_of(owner * (depth // 2), 16), depth // 2)
        buf, start, count = places[p]
        return weights.at[buf, shard, at, pl.ds(start, count)]

    def send_part(p, shard, kind, role, dev):
        ref = part(p, shard, kind)
        send(ref, ref, weight_sem.at[p, role], dev)

    def to_other_core(p, at):
        shard, role = peer_role[at]
        ref = side(p, shard, core)
        send(ref, ref, weight_sem.at[p, PEER + role], to_peer)

    def wait_part(p, shard, kind, role):
        await_copy(part(p, shard, kind), weight_sem.at[p, role])

    def wait_side(p, shard, role):
        await_copy(side(p, shard, core), weight_sem.at[p, role])

    to_y = (to_pair, to_cross)

    def a1(p):
        low, high = p % 2, 1 - p % 2
        wait_part(p, down_own, low, DN + low)
        send_part(p, down_own, low, FAR, to_up)
        send_part(p, down_own, low, DNO, to_y[low])
        wait_part(p, up_own, high, UP + high)
        send_part(p, up_own, high, FAR, to_down)
        send_part(p, up_own, high, UPO, to_y[high])

    def a2(p):
        low, high = p % 2, 1 - p % 2
        wait_part(p, down_own, high, DN + high)
        send_part(p, down_own, high, DNO, to_y[high])
        to_other_core(p, 0)
        wait_part(p, up_own, low, UP + low)
        send_part(p, up_own, low, UPO, to_y[low])
        to_other_core(p, 1)

    def a3(p):
        wait_side(p, far_own, FAR)
        send_part(p, far_own, A, FARO, to_pair)
        send_part(p, far_own, B, FARO, to_cross)
        to_other_core(p, 2)

    def y0(p):
        wait_side(p, pair, PAIR)
        to_other_core(p, 3)

    def y2(p):
        wait_side(p, down_oth, DNO)
        to_other_core(p, 4)
        wait_side(p, up_oth, UPO)
        to_other_core(p, 5)

    def y3(p):
        wait_side(p, far_oth, FARO)
        to_other_core(p, 6)

    def first_z(p):
        low, high = p % 2, 1 - p % 2
        send_part(p, own, low, DN + low, to_up)
        send_part(p, own, high, UP + high, to_down)

    def second_z(p):
        low, high = p % 2, 1 - p % 2
        send_part(p, own, high, DN + high, to_up)
        send_part(p, own, low, UP + low, to_down)

    def start_z(p):
        first_z(p)
        second_z(p)

    def start_y(p):
        send_part(p, own, A, PAIR, to_pair)
        send_part(p, own, B, PAIR, to_cross)

    def finish(p, *at):
        for i in at:
            shard, role = peer_role[i]
            await_copy(side(p, shard, 1 - core), weight_sem.at[p, PEER + role])
        add(p, *[peer_role[i][0] for i in at])

    dn_, up_, far_, pair_, dno_, upo_, faro_ = range(7)

    first_z(0)
    start_y(0)
    second_z(0)
    loaded(pos_ref, 6)
    posb[ctx] = jnp.broadcast_to(pos_ref[...].reshape(1, rows), (8, rows)).astype(jnp.float32)
    loaded(weights.at[2, ctx], 2)
    start_y(1)

    loaded(xv, 4)
    loaded(gain_ref, 5)
    loaded(freq_ref, 7)
    block = 64
    gain = gain_ref[...].reshape(1, feats)

    @pl.loop(0, rows // block)
    def _(i):
        at = tile(i, block)
        value = xv[at, :].astype(jnp.float32)
        scale = lax.rsqrt(jnp.mean(value * value, -1, keepdims=True) + 1e-06)
        out = (value * scale * gain).astype(jnp.bfloat16)
        for s in range(SHARDS):
            normed[s, at, :] = out[:, s * depth : (s + 1) * depth]

    loaded(weights.at[1, ctx], 1)
    loaded(weights.at[3, ctx], 3)

    def angles():
        angle = jnp.transpose(posb[ctx])[:, :1] * freq_ref[...]
        k = jnp.floor(angle * (2.0 / math.pi) + 0.5)
        t = angle - k * 1.5703125
        t = t - k * 4.8375129699707031e-4
        t = t - k * 7.5497899548918822e-8
        q = k - 4.0 * jnp.floor(k * 0.25)
        s = t * t
        sin = t + t * s * (-1.6666654611e-1 + s * (8.3321608736e-3 - s * 1.9515295891e-4))
        cos = 1.0 - 0.5 * s + s * s * (
            4.166664568298827e-2 + s * (s * 2.443315711809948e-5 - 1.388731625493765e-3)
        )
        odd = (q == 1.0) | (q == 3.0)
        sine = jnp.where(odd, cos, sin)
        cosine = jnp.where(odd, sin, cos)
        lane = lax.broadcasted_iota(jnp.int32, sine.shape, 1)
        sin_ref[...] = jnp.where((q >= 2.0) ^ (lane < hd // 2), -sine, sine)
        cos_ref[...] = jnp.where((q == 1.0) | (q == 2.0), -cosine, cosine)

    def rope(u):
        return u * cos_ref[...] + pltpu.roll(u, hd // 2, 1) * sin_ref[...]

    def keys_values(j):
        for ref, base in ((kvb.at[ctx], par), (kvx, other)):
            ref[j, :, :hd] = rope(acc[j, :, tile(base, hd)]).astype(jnp.bfloat16)
            ref[j, :, hd:] = acc[j, :, tile(2 + base, hd)].astype(jnp.bfloat16)

    def query(j, r):
        at = slice(r * rows, (r + 1) * rows)
        for ref, base in ((qx, other), (qb.at[0], par)):
            u = acc[2 + j, :, tile(2 * r + base, hd)]
            ref[j, at, :] = (rope(u) * query_scale).astype(jnp.bfloat16)
        send(qx.at[j, at, :], qb.at[1, j, at, :], q_sem.at[j, r], to_pair)

    def query_wait(j, r):
        at = slice(r * rows, (r + 1) * rows)
        await_copy(qb.at[1, j, at, :], q_sem.at[j, r])

    def kv_half(blk, j, half):
        return kvb.at[blk, j, pl.ds(half * half_rows, half_rows), :]

    def kv_send(blk, j, half, role, dev):
        ref = kv_half(blk, j, half)
        send(ref, ref, kv_sem.at[j, role], dev)

    def kv_to_pair(j):
        send(kvx.at[j], kvb.at[ctx, j], kv_sem.at[j, 0], to_pair)

    def kv_to_z(blk, j, base):
        for half in range(2):
            kv_send(blk, j, half, base + half, to_up)
            kv_send(blk, j, 1 - half, base + 2 + 1 - half, to_down)

    def kv_pair(j):
        await_copy(kvb.at[pair, j], kv_sem.at[j, 0])
        kv_to_z(pair, j, 6)

    def kv_relay(low, high, j, base):
        await_copy(kv_half(low, j, 0), kv_sem.at[j, base])
        kv_send(low, j, 0, base + 4, to_up)
        await_copy(kv_half(high, j, 1), kv_sem.at[j, base + 3])
        kv_send(high, j, 1, base + 4, to_down)
        await_copy(kv_half(low, j, 1), kv_sem.at[j, base + 1])
        await_copy(kv_half(high, j, 0), kv_sem.at[j, base + 2])

    def unit(src, j, step):
        zr = (z + step + step // 2 - 2 * (step // 3)) % 4
        blocks = pl.ds(zr * 2, 2)
        kk = kvb[blocks, j, :, :hd].reshape(2 * rows, hd)
        vv = kvb[blocks, j, :, hd:].reshape(2 * rows, hd)
        vv = jnp.concatenate([vv, jnp.ones_like(vv)], 1)
        kp = jnp.concatenate([posb[zr * 2, :1, :], posb[zr * 2 + 1, :1, :]], 1)
        s = lax.dot_general(
            qb[src, j], kk, (((1,), (1,)), ((), ())), preferred_element_type=jnp.float32
        )
        w = jnp.exp2(jnp.tanh(s * 0.02) * EXP_SCALE)
        w = jnp.where(kp <= qpos[src], w, 0.0).astype(jnp.bfloat16)
        num[src, j] += jnp.dot(w, vv, preferred_element_type=jnp.float32)

    def result(src, j, r):
        n = num[src, j, r * rows : (r + 1) * rows, :]
        return (n[:, :hd] / n[:, hd:]).astype(jnp.bfloat16)

    def columns(base, h):
        return o_hbm.at[:, tile(base * 4 + h, hd)]

    def give_back(j, r):
        h = 2 * j + r
        osend[h] = result(1, j, r)
        send(osend.at[h], columns(par, h), o_sem.at[0], to_pair)

    def keep(j, r):
        h = 2 * j + r
        oown[h] = result(0, j, r)
        pltpu.make_async_copy(oown.at[h], columns(par, h), out_sem.at[0]).start()

    def far_wait(j):
        await_copy(kvb.at[far_own, j], kv_sem.at[j, 5])
        await_copy(kvb.at[far_oth, j], kv_sem.at[j, 10])

    add(0, own, first=True)
    for dev in group:
        send(posb.at[ctx], posb.at[ctx], pos_sem.at[0], dev)
    angles()
    a1(0)
    start_z(1)
    y0(0)
    num[...] = jnp.zeros_like(num)
    a2(0)
    y0(1)
    finish(0, pair_)
    a3(0)
    finish(0, dn_, up_)
    a1(1)
    start_z(2)
    y2(0)
    add(1, own, first=True)
    finish(1, pair_)
    a2(1)
    y3(0)
    finish(0, dno_, upo_, far_)
    finish(0, faro_)
    keys_values(0)
    a3(1)
    kv_to_pair(0)
    kv_to_z(ctx, 0, 1)
    start_y(2)
    finish(1, dn_, up_)
    a1(2)
    start_z(3)
    y2(1)
    add(2, own, first=True)
    a2(2)
    await_copy(posb.at[pl.ds(0, SHARDS - 1)], pos_sem.at[0])
    for src, blk in ((0, ctx), (1, pair)):
        col = jnp.transpose(posb[blk])[:, :1]
        for r in range(2):
            qpos[src, r * rows : (r + 1) * rows, :] = col
    finish(1, dno_, upo_, far_)
    y3(1)
    finish(1, faro_)
    query(0, 0)
    query(0, 1)
    kv_relay(down_own, up_own, 0, 1)

    def before_0():
        kv_pair(0)

    def before_1():
        start_y(3)
        y0(2)
        a3(2)
        finish(2, pair_, dn_, up_)
        a1(3)
        a2(3)
        start_z(4)
        start_y(4)
        y2(2)
        finish(2, dno_, upo_, far_)
        query_wait(0, 0)
        query_wait(0, 1)

    def before_2():
        kv_relay(down_oth, up_oth, 0, 6)
        y0(3)

    def before_3():
        a3(3)
        y3(2)
        a1(4)
        finish(2, faro_)
        keys_values(1)
        kv_to_pair(1)
        a2(4)

    def before_4():
        kv_to_z(ctx, 1, 1)
        add(3, own, first=True)
        finish(3, pair_, dn_, up_)
        y2(3)

    def before_5():
        a3(4)
        y3(3)
        finish(3, dno_, upo_, far_)
        add(4, own, first=True)
        y0(4)
        finish(3, faro_)
        query(1, 0)
        finish(4, pair_, dn_, up_)
        y2(4)
        y3(4)
        kv_pair(1)
        finish(4, dno_, upo_, far_)
        finish(4, faro_)
        query(1, 1)

    def before_6():
        kv_relay(down_own, up_own, 1, 1)
        far_wait(0)

    def before_7():
        give_back(0, 0)
        give_back(0, 1)

    def before_8():
        keep(0, 0)
        keep(0, 1)

    def before_9():
        kv_relay(down_oth, up_oth, 1, 6)
        query_wait(1, 0)
        query_wait(1, 1)

    def before_13():
        give_back(1, 0)
        give_back(1, 1)

    before = {
        0: before_0, 1: before_1, 2: before_2, 3: before_3, 4: before_4, 5: before_5,
        6: before_6, 7: before_7, 8: before_8, 9: before_9,
        12: lambda: far_wait(1), 13: before_13,
    }

    @pl.loop(0, 16)
    def _(t):
        for at, action in before.items():
            pl.when(t == at)(action)
        j, u = t // 8, t % 8
        past = (u + 3) // 8
        late = (u + 3) // 4 - 2 * past
        theirs = (1 - j) * ((u % 2 + u // 6) % 2) + j * late
        unit(theirs, j, (1 - j) * (u // 2) + j * (u - late - 4 * past))

    keep(1, 0)
    keep(1, 1)
    mine = o_hbm.at[:, tile(par, 4 * hd)]
    pltpu.make_async_copy(mine, mine, out_sem.at[0]).wait()
    await_copy(o_hbm.at[:, tile(other, 4 * hd)], o_sem.at[0])
    for at in range(len(sends) - SENDS, len(sends)):
        sent(at)


def on_device(tokens, token_pos, norm_gain, query_weight, key_weight, value_weight):
    rows, feats = tokens.shape
    depth, nq = query_weight.shape
    nk = key_weight.shape[1]
    half = HEAD_DIM // 2
    freq = (10000.0 ** (-np.arange(half) * 2.0 / HEAD_DIM)).astype(np.float32)
    freq = jnp.asarray(np.concatenate([freq, freq])[None, :])
    hbm = pl.BlockSpec(memory_space=pl.ANY)
    bf16, f32 = jnp.bfloat16, jnp.float32
    dma = pltpu.SemaphoreType.DMA
    return pl.pallas_call(
        kernel,
        out_shape=jax.ShapeDtypeStruct((rows, nq), bf16),
        in_specs=[hbm] * 7,
        out_specs=hbm,
        scratch_shapes=[
            pltpu.VMEM((feats,), f32),
            pltpu.VMEM((1, HEAD_DIM), f32),
            pltpu.VMEM((rows,), jnp.int32),
            pltpu.VMEM((rows, HEAD_DIM), f32),
            pltpu.VMEM((rows, HEAD_DIM), f32),
            pltpu.VMEM((rows, feats), bf16),
            pltpu.VMEM((SHARDS, rows, depth), bf16),
            pltpu.VMEM((4, SHARDS, depth, nk), bf16),
            pltpu.VMEM((4, rows, nk), f32),
            pltpu.VMEM((SHARDS, 8, rows), f32),
            pltpu.VMEM((2, 2 * rows, 1), f32),
            pltpu.VMEM((SHARDS, 2, rows, 2 * HEAD_DIM), bf16),
            pltpu.VMEM((2, rows, 2 * HEAD_DIM), bf16),
            pltpu.VMEM((2, 2, 2 * rows, HEAD_DIM), bf16),
            pltpu.VMEM((2, 2 * rows, HEAD_DIM), bf16),
            pltpu.VMEM((2, 2, 2 * rows, 2 * HEAD_DIM), f32),
            pltpu.VMEM((4, rows, HEAD_DIM), bf16),
            pltpu.VMEM((4, rows, HEAD_DIM), bf16),
            dma((8,)),
            dma((1,)),
            dma((SENDS,)),
            dma((5, 16)),
            dma((2, 11)),
            dma((2, 2)),
            dma((1,)),
            dma((1,)),
        ],
        compiler_params=pltpu.CompilerParams(
            collective_id=0, has_side_effects=True, vmem_limit_bytes=62 * 1024 * 1024
        ),
        name="block",
    )(
        tokens, norm_gain, query_weight, key_weight, value_weight, freq, token_pos,
    )


def solution(mesh):
    in_specs = (
        P(("grp", "ctx"), None),
        P(("grp", "ctx")),
        P(),
        P("ctx", "tp"),
        P("ctx", "tp"),
        P("ctx", "tp"),
    )
    out_specs = P(("grp", "ctx"), "tp")
    return jax.shard_map(
        on_device, mesh=mesh, in_specs=in_specs, out_specs=out_specs, check_vma=False
    )
```

```python
import functools
import math

import jax
import jax.numpy as jnp
import numpy as np
from jax import lax
from jax.experimental import pallas as pl
from jax.experimental.pallas import tpu as pltpu
from jax.sharding import PartitionSpec as P

HEAD_DIM = 128
MESH = pl.DeviceIdType.MESH
query_scale = 144.0 ** (-0.5)
EXP_SCALE = 50.0 * math.log2(math.e)
SHARDS = 8
SENDS = 64
SPLITS = (128, 112, 112, 112, 112)


def tile(index, size):
    return pl.ds(pl.multiple_of(index * size, size), size)


def kernel(
    x_hbm, gain_hbm, wq_hbm, wk_hbm, wv_hbm, freq_hbm, pos_hbm,
    o_hbm,
    gain_ref, freq_ref, pos_ref, cos_ref, sin_ref, xv, normed, weights, acc, posb, qpos, kvb, kvx, qb, qx, num, oown, osend,
    local_sem, out_sem, send_sem, weight_sem, kv_sem, q_sem, o_sem, pos_sem,
):
    ctx = lax.axis_index("ctx")
    grp = lax.axis_index("grp")
    z, par = ctx // 2, ctx % 2
    y_hi, core = grp // 2, grp % 2
    up, down, far = (z + 1) % 4, (z + 3) % 4, (z + 2) % 4
    other = 1 - par
    pair = z * 2 + other
    to_up = {"ctx": up * 2 + par}
    to_down = {"ctx": down * 2 + par}
    to_pair = {"ctx": pair}
    to_cross = {"ctx": pair, "grp": (1 - y_hi) * 2 + core}
    to_peer = {"grp": y_hi * 2 + (1 - core)}
    group = [{"ctx": (ctx + i) % SHARDS} for i in range(1, SHARDS)]

    rows, feats = xv.shape
    depth = weights.shape[2]
    nq, nk = wq_hbm.shape[1], wk_hbm.shape[1]
    hd = HEAD_DIM
    half_rows = rows // 2

    barrier = pltpu.get_barrier_semaphore()
    for dev in group + [to_cross, to_peer]:
        pl.semaphore_signal(barrier, inc=1, device_id=dev, device_id_type=MESH)
    def load(src, dst, at):
        pltpu.make_async_copy(src, dst, local_sem.at[at]).start()

    def loaded(dst, at):
        pltpu.make_async_copy(dst, dst, local_sem.at[at]).wait()

    def load_kv(j):
        for i in range(2):
            for at, ref in ((i, wk_hbm), (2 + i, wv_hbm)):
                load(
                    ref.at[:, pl.ds((2 * i + j) * hd, hd)],
                    weights.at[j, ctx, :, pl.ds(at * hd, hd)],
                    j,
                )

    def load_q(j):
        for r in range(2):
            for i in range(2):
                load(
                    wq_hbm.at[:, pl.ds((4 * i + 2 * j + r) * hd, hd)],
                    weights.at[2 + j, ctx, :, pl.ds((2 * r + i) * hd, hd)],
                    2 + j,
                )

    load_kv(0)
    load(x_hbm, xv, 4)
    load(gain_hbm, gain_ref, 5)
    load(pos_hbm, pos_ref, 6)
    load(freq_hbm, freq_ref, 7)
    load_q(0)
    load_kv(1)
    load_q(1)
    loaded(weights.at[0, ctx], 0)
    pl.semaphore_wait(barrier, SHARDS + 1)

    sends = []

    def copy_of(src, dst, recv, dev, at):
        return pltpu.make_async_remote_copy(
            src_ref=src, dst_ref=dst, send_sem=send_sem.at[at % SENDS], recv_sem=recv,
            device_id=dev, device_id_type=MESH,
        )

    def sent(at):
        count, width = sends[at]
        ref = weights.at[0, 0, pl.ds(0, count), pl.ds(0, width)]
        copy_of(ref, ref, weight_sem.at[0, 0], to_peer, at).wait_send()

    def send(src, dst, recv, dev):
        if len(sends) >= SENDS:
            sent(len(sends) - SENDS)
        copy_of(src, dst, recv, dev, len(sends)).start()
        count, width = src.shape[-2:]
        sends.append((count * src.dtype.itemsize // 2, width))

    def await_copy(dst, recv):
        copy_of(dst, dst, recv, to_peer, 0).wait_recv()

    A, B = 0, 1
    own = ctx
    up_own, up_oth = up * 2 + par, up * 2 + other
    down_own, down_oth = down * 2 + par, down * 2 + other
    far_own, far_oth = far * 2 + par, far * 2 + other

    places = [(0, 0, nk), (2, 0, nk), (1, 0, nk), (3, 0, nk // 2), (3, nk // 2, nk // 2)]

    def add(p, *shards, first=False):
        buf, start, count = places[p]
        width = 256

        @pl.loop(0, count // width)
        def _(i):
            cols = pl.ds(pl.multiple_of(start + i * width, width), width)
            part = sum(
                jnp.dot(normed[s], weights[buf, s, :, cols], preferred_element_type=jnp.float32)
                for s in shards
            )
            acc[buf, :, cols] = part if first else acc[buf, :, cols] + part

    DN, UP, FAR, PAIR, DNO, UPO, FARO, PEER = 0, 2, 4, 5, 6, 7, 8, 9
    peer_role = [(down_own, 0), (up_own, 1), (far_own, 2), (pair, 3)]
    peer_role += [(down_oth, 4), (up_oth, 5), (far_oth, 6)]

    def part(p, shard, kind):
        base = core * (depth // 2) + (SPLITS[p] if kind else 0)
        size = depth // 2 - SPLITS[p] if kind else SPLITS[p]
        buf, start, count = places[p]
        return weights.at[buf, shard, pl.ds(pl.multiple_of(base, 16), size), pl.ds(start, count)]

    def side(p, shard, owner):
        at = pl.ds(pl.multiple_of(owner * (depth // 2), 16), depth // 2)
        buf, start, count = places[p]
        return weights.at[buf, shard, at, pl.ds(start, count)]

    def send_part(p, shard, kind, role, dev):
        ref = part(p, shard, kind)
        send(ref, ref, weight_sem.at[p, role], dev)

    def to_other_core(p, at):
        shard, role = peer_role[at]
        ref = side(p, shard, core)
        send(ref, ref, weight_sem.at[p, PEER + role], to_peer)

    def wait_part(p, shard, kind, role):
        await_copy(part(p, shard, kind), weight_sem.at[p, role])

    def wait_side(p, shard, role):
        await_copy(side(p, shard, core), weight_sem.at[p, role])

    to_y = (to_pair, to_cross)

    def a1(p):
        low, high = p % 2, 1 - p % 2
        wait_part(p, down_own, low, DN + low)
        send_part(p, down_own, low, FAR, to_up)
        send_part(p, down_own, low, DNO, to_y[low])
        wait_part(p, up_own, high, UP + high)
        send_part(p, up_own, high, FAR, to_down)
        send_part(p, up_own, high, UPO, to_y[high])

    def a2(p):
        low, high = p % 2, 1 - p % 2
        wait_part(p, down_own, high, DN + high)
        send_part(p, down_own, high, DNO, to_y[high])
        to_other_core(p, 0)
        wait_part(p, up_own, low, UP + low)
        send_part(p, up_own, low, UPO, to_y[low])
        to_other_core(p, 1)

    def a3(p):
        wait_side(p, far_own, FAR)
        send_part(p, far_own, A, FARO, to_pair)
        send_part(p, far_own, B, FARO, to_cross)
        to_other_core(p, 2)

    def y0(p):
        wait_side(p, pair, PAIR)
        to_other_core(p, 3)

    def y2(p):
        wait_side(p, down_oth, DNO)
        to_other_core(p, 4)
        wait_side(p, up_oth, UPO)
        to_other_core(p, 5)

    def y3(p):
        wait_side(p, far_oth, FARO)
        to_other_core(p, 6)

    def first_z(p):
        low, high = p % 2, 1 - p % 2
        send_part(p, own, low, DN + low, to_up)
        send_part(p, own, high, UP + high, to_down)

    def second_z(p):
        low, high = p % 2, 1 - p % 2
        send_part(p, own, high, DN + high, to_up)
        send_part(p, own, low, UP + low, to_down)

    def start_z(p):
        first_z(p)
        second_z(p)

    def start_y(p):
        send_part(p, own, A, PAIR, to_pair)
        send_part(p, own, B, PAIR, to_cross)

    def finish(p, *at):
        for i in at:
            shard, role = peer_role[i]
            await_copy(side(p, shard, 1 - core), weight_sem.at[p, PEER + role])
        add(p, *[peer_role[i][0] for i in at])

    dn_, up_, far_, pair_, dno_, upo_, faro_ = range(7)

    first_z(0)
    start_y(0)
    second_z(0)
    loaded(pos_ref, 6)
    posb[ctx] = jnp.broadcast_to(pos_ref[...].reshape(1, rows), (8, rows)).astype(jnp.float32)
    loaded(weights.at[2, ctx], 2)
    start_y(1)

    loaded(xv, 4)
    loaded(gain_ref, 5)
    loaded(freq_ref, 7)
    block = 64
    gain = gain_ref[...].reshape(1, feats)

    @pl.loop(0, rows // block)
    def _(i):
        at = tile(i, block)
        value = xv[at, :].astype(jnp.float32)
        scale = lax.rsqrt(jnp.mean(value * value, -1, keepdims=True) + 1e-06)
        out = (value * scale * gain).astype(jnp.bfloat16)
        for s in range(SHARDS):
            normed[s, at, :] = out[:, s * depth : (s + 1) * depth]

    loaded(weights.at[1, ctx], 1)
    loaded(weights.at[3, ctx], 3)

    def angles():
        angle = jnp.transpose(posb[ctx])[:, :1] * freq_ref[...]
        k = jnp.floor(angle * (2.0 / math.pi) + 0.5)
        t = angle - k * 1.5703125
        t = t - k * 4.8375129699707031e-4
        t = t - k * 7.5497899548918822e-8
        q = k - 4.0 * jnp.floor(k * 0.25)
        s = t * t
        sin = t + t * s * (-1.6666654611e-1 + s * (8.3321608736e-3 - s * 1.9515295891e-4))
        cos = 1.0 - 0.5 * s + s * s * (
            4.166664568298827e-2 + s * (s * 2.443315711809948e-5 - 1.388731625493765e-3)
        )
        odd = (q == 1.0) | (q == 3.0)
        sine = jnp.where(odd, cos, sin)
        cosine = jnp.where(odd, sin, cos)
        lane = lax.broadcasted_iota(jnp.int32, sine.shape, 1)
        sin_ref[...] = jnp.where((q >= 2.0) ^ (lane < hd // 2), -sine, sine)
        cos_ref[...] = jnp.where((q == 1.0) | (q == 2.0), -cosine, cosine)

    def rope(u):
        return u * cos_ref[...] + pltpu.roll(u, hd // 2, 1) * sin_ref[...]

    def keys_values(j):
        for ref, base in ((kvb.at[ctx], par), (kvx, other)):
            ref[j, :, :hd] = rope(acc[j, :, tile(base, hd)]).astype(jnp.bfloat16)
            ref[j, :, hd:] = acc[j, :, tile(2 + base, hd)].astype(jnp.bfloat16)

    def query(j, r):
        at = slice(r * rows, (r + 1) * rows)
        for ref, base in ((qx, other), (qb.at[0], par)):
            u = acc[2 + j, :, tile(2 * r + base, hd)]
            ref[j, at, :] = (rope(u) * query_scale).astype(jnp.bfloat16)
        send(qx.at[j, at, :], qb.at[1, j, at, :], q_sem.at[j, r], to_pair)

    def query_wait(j, r):
        at = slice(r * rows, (r + 1) * rows)
        await_copy(qb.at[1, j, at, :], q_sem.at[j, r])

    def kv_half(blk, j, half):
        return kvb.at[blk, j, pl.ds(half * half_rows, half_rows), :]

    def kv_send(blk, j, half, role, dev):
        ref = kv_half(blk, j, half)
        send(ref, ref, kv_sem.at[j, role], dev)

    def kv_to_pair(j):
        send(kvx.at[j], kvb.at[ctx, j], kv_sem.at[j, 0], to_pair)

    def kv_to_z(blk, j, base):
        for half in range(2):
            kv_send(blk, j, half, base + half, to_up)
            kv_send(blk, j, 1 - half, base + 2 + 1 - half, to_down)

    def kv_pair(j):
        await_copy(kvb.at[pair, j], kv_sem.at[j, 0])
        kv_to_z(pair, j, 6)

    def kv_relay(low, high, j, base):
        await_copy(kv_half(low, j, 0), kv_sem.at[j, base])
        kv_send(low, j, 0, base + 4, to_up)
        await_copy(kv_half(high, j, 1), kv_sem.at[j, base + 3])
        kv_send(high, j, 1, base + 4, to_down)
        await_copy(kv_half(low, j, 1), kv_sem.at[j, base + 1])
        await_copy(kv_half(high, j, 0), kv_sem.at[j, base + 2])

    def unit(src, j, step):
        zr = (z + step + step // 2 - 2 * (step // 3)) % 4
        blocks = pl.ds(zr * 2, 2)
        kk = kvb[blocks, j, :, :hd].reshape(2 * rows, hd)
        vv = kvb[blocks, j, :, hd:].reshape(2 * rows, hd)
        vv = jnp.concatenate([vv, jnp.ones_like(vv)], 1)
        kp = jnp.concatenate([posb[zr * 2, :1, :], posb[zr * 2 + 1, :1, :]], 1)
        s = lax.dot_general(
            qb[src, j], kk, (((1,), (1,)), ((), ())), preferred_element_type=jnp.float32
        )
        w = jnp.exp2(jnp.tanh(s * 0.02) * EXP_SCALE)
        w = jnp.where(kp <= qpos[src], w, 0.0).astype(jnp.bfloat16)
        num[src, j] += jnp.dot(w, vv, preferred_element_type=jnp.float32)

    def result(src, j, r):
        n = num[src, j, r * rows : (r + 1) * rows, :]
        return (n[:, :hd] / n[:, hd:]).astype(jnp.bfloat16)

    def columns(base, h):
        return o_hbm.at[:, tile(base * 4 + h, hd)]

    def give_back(j, r):
        h = 2 * j + r
        osend[h] = result(1, j, r)
        send(osend.at[h], columns(par, h), o_sem.at[0], to_pair)

    def keep(j, r):
        h = 2 * j + r
        oown[h] = result(0, j, r)
        pltpu.make_async_copy(oown.at[h], columns(par, h), out_sem.at[0]).start()

    def far_wait(j):
        await_copy(kvb.at[far_own, j], kv_sem.at[j, 5])
        await_copy(kvb.at[far_oth, j], kv_sem.at[j, 10])

    add(0, own, first=True)
    for dev in group:
        send(posb.at[ctx], posb.at[ctx], pos_sem.at[0], dev)
    angles()
    a1(0)
    start_z(1)
    y0(0)
    num[...] = jnp.zeros_like(num)
    a2(0)
    y0(1)
    finish(0, pair_)
    a3(0)
    finish(0, dn_, up_)
    a1(1)
    start_z(2)
    y2(0)
    add(1, own, first=True)
    finish(1, pair_)
    a2(1)
    y3(0)
    finish(0, dno_, upo_, far_)
    finish(0, faro_)
    keys_values(0)
    a3(1)
    kv_to_pair(0)
    kv_to_z(ctx, 0, 1)
    start_y(2)
    finish(1, dn_, up_)
    a1(2)
    start_z(3)
    y2(1)
    add(2, own, first=True)
    a2(2)
    await_copy(posb.at[pl.ds(0, SHARDS - 1)], pos_sem.at[0])
    for src, blk in ((0, ctx), (1, pair)):
        col = jnp.transpose(posb[blk])[:, :1]
        for r in range(2):
            qpos[src, r * rows : (r + 1) * rows, :] = col
    finish(1, dno_, upo_, far_)
    y3(1)
    finish(1, faro_)
    query(0, 0)
    query(0, 1)
    kv_relay(down_own, up_own, 0, 1)

    def before_0():
        kv_pair(0)

    def before_1():
        start_y(3)
        y0(2)
        a3(2)
        finish(2, pair_, dn_, up_)
        a1(3)
        a2(3)
        start_z(4)
        start_y(4)
        y2(2)
        finish(2, dno_, upo_, far_)
        query_wait(0, 0)
        query_wait(0, 1)

    def before_2():
        kv_relay(down_oth, up_oth, 0, 6)
        y0(3)

    def before_3():
        a3(3)
        y3(2)
        a1(4)
        finish(2, faro_)
        keys_values(1)
        kv_to_pair(1)
        kv_to_z(ctx, 1, 1)
        a2(4)

    def before_4():
        add(3, own, first=True)
        finish(3, pair_, dn_, up_)
        y2(3)

    def before_5():
        a3(4)
        y3(3)
        finish(3, dno_, upo_, far_)
        add(4, own, first=True)
        y0(4)
        finish(3, faro_)
        query(1, 0)
        finish(4, pair_, dn_, up_)
        y2(4)
        y3(4)
        kv_pair(1)
        finish(4, dno_, upo_, far_)
        finish(4, faro_)
        query(1, 1)

    def before_6():
        kv_relay(down_own, up_own, 1, 1)
        far_wait(0)

    def before_7():
        give_back(0, 0)
        give_back(0, 1)

    def before_8():
        keep(0, 0)
        keep(0, 1)

    def before_9():
        kv_relay(down_oth, up_oth, 1, 6)
        query_wait(1, 0)
        query_wait(1, 1)

    def before_13():
        give_back(1, 0)
        give_back(1, 1)

    before = {
        0: before_0, 1: before_1, 2: before_2, 3: before_3, 4: before_4, 5: before_5,
        6: before_6, 7: before_7, 8: before_8, 9: before_9,
        12: lambda: far_wait(1), 13: before_13,
    }

    @pl.loop(0, 16)
    def _(t):
        for at, action in before.items():
            pl.when(t == at)(action)
        j, u = t // 8, t % 8
        past = (u + 3) // 8
        late = (u + 3) // 4 - 2 * past
        theirs = (1 - j) * ((u % 2 + u // 6) % 2) + j * late
        unit(theirs, j, (1 - j) * (u // 2) + j * (u - late - 4 * past))

    keep(1, 0)
    keep(1, 1)
    mine = o_hbm.at[:, tile(par, 4 * hd)]
    pltpu.make_async_copy(mine, mine, out_sem.at[0]).wait()
    await_copy(o_hbm.at[:, tile(other, 4 * hd)], o_sem.at[0])
    for at in range(len(sends) - SENDS, len(sends)):
        sent(at)


def on_device(tokens, token_pos, norm_gain, query_weight, key_weight, value_weight):
    rows, feats = tokens.shape
    depth, nq = query_weight.shape
    nk = key_weight.shape[1]
    half = HEAD_DIM // 2
    freq = (10000.0 ** (-np.arange(half) * 2.0 / HEAD_DIM)).astype(np.float32)
    freq = jnp.asarray(np.concatenate([freq, freq])[None, :])
    hbm = pl.BlockSpec(memory_space=pl.ANY)
    bf16, f32 = jnp.bfloat16, jnp.float32
    dma = pltpu.SemaphoreType.DMA
    return pl.pallas_call(
        kernel,
        out_shape=jax.ShapeDtypeStruct((rows, nq), bf16),
        in_specs=[hbm] * 7,
        out_specs=hbm,
        scratch_shapes=[
            pltpu.VMEM((feats,), f32),
            pltpu.VMEM((1, HEAD_DIM), f32),
            pltpu.VMEM((rows,), jnp.int32),
            pltpu.VMEM((rows, HEAD_DIM), f32),
            pltpu.VMEM((rows, HEAD_DIM), f32),
            pltpu.VMEM((rows, feats), bf16),
            pltpu.VMEM((SHARDS, rows, depth), bf16),
            pltpu.VMEM((4, SHARDS, depth, nk), bf16),
            pltpu.VMEM((4, rows, nk), f32),
            pltpu.VMEM((SHARDS, 8, rows), f32),
            pltpu.VMEM((2, 2 * rows, 1), f32),
            pltpu.VMEM((SHARDS, 2, rows, 2 * HEAD_DIM), bf16),
            pltpu.VMEM((2, rows, 2 * HEAD_DIM), bf16),
            pltpu.VMEM((2, 2, 2 * rows, HEAD_DIM), bf16),
            pltpu.VMEM((2, 2 * rows, HEAD_DIM), bf16),
            pltpu.VMEM((2, 2, 2 * rows, 2 * HEAD_DIM), f32),
            pltpu.VMEM((4, rows, HEAD_DIM), bf16),
            pltpu.VMEM((4, rows, HEAD_DIM), bf16),
            dma((8,)),
            dma((1,)),
            dma((SENDS,)),
            dma((5, 16)),
            dma((2, 11)),
            dma((2, 2)),
            dma((1,)),
            dma((1,)),
        ],
        compiler_params=pltpu.CompilerParams(
            collective_id=0, has_side_effects=True, vmem_limit_bytes=62 * 1024 * 1024
        ),
        name="block",
    )(
        tokens, norm_gain, query_weight, key_weight, value_weight, freq, token_pos,
    )


def solution(mesh):
    in_specs = (
        P(("grp", "ctx"), None),
        P(("grp", "ctx")),
        P(),
        P("ctx", "tp"),
        P("ctx", "tp"),
        P("ctx", "tp"),
    )
    out_specs = P(("grp", "ctx"), "tp")
    return jax.shard_map(
        on_device, mesh=mesh, in_specs=in_specs, out_specs=out_specs, check_vma=False
    )
```

```python
import functools
import math

import jax
import jax.numpy as jnp
import numpy as np
from jax import lax
from jax.experimental import pallas as pl
from jax.experimental.pallas import tpu as pltpu
from jax.sharding import PartitionSpec as P

HEAD_DIM = 128
MESH = pl.DeviceIdType.MESH
query_scale = 144.0 ** (-0.5)
EXP_SCALE = 50.0 * math.log2(math.e)
SHARDS = 8
SENDS = 64
SPLITS = (128, 112, 96, 112, 112)


def tile(index, size):
    return pl.ds(pl.multiple_of(index * size, size), size)


def kernel(
    x_hbm, gain_hbm, wq_hbm, wk_hbm, wv_hbm, freq_hbm, pos_hbm,
    o_hbm,
    gain_ref, freq_ref, pos_ref, cos_ref, sin_ref, xv, normed, weights, acc, posb, qpos, kvb, kvx, qb, qx, num, oown, osend,
    local_sem, out_sem, send_sem, weight_sem, kv_sem, q_sem, o_sem, pos_sem,
):
    ctx = lax.axis_index("ctx")
    grp = lax.axis_index("grp")
    z, par = ctx // 2, ctx % 2
    y_hi, core = grp // 2, grp % 2
    up, down, far = (z + 1) % 4, (z + 3) % 4, (z + 2) % 4
    other = 1 - par
    pair = z * 2 + other
    to_up = {"ctx": up * 2 + par}
    to_down = {"ctx": down * 2 + par}
    to_pair = {"ctx": pair}
    to_cross = {"ctx": pair, "grp": (1 - y_hi) * 2 + core}
    to_peer = {"grp": y_hi * 2 + (1 - core)}
    group = [{"ctx": (ctx + i) % SHARDS} for i in range(1, SHARDS)]

    rows, feats = xv.shape
    depth = weights.shape[2]
    nq, nk = wq_hbm.shape[1], wk_hbm.shape[1]
    hd = HEAD_DIM
    half_rows = rows // 2

    barrier = pltpu.get_barrier_semaphore()
    for dev in group + [to_cross, to_peer]:
        pl.semaphore_signal(barrier, inc=1, device_id=dev, device_id_type=MESH)
    def load(src, dst, at):
        pltpu.make_async_copy(src, dst, local_sem.at[at]).start()

    def loaded(dst, at):
        pltpu.make_async_copy(dst, dst, local_sem.at[at]).wait()

    def load_kv(j):
        for i in range(2):
            for at, ref in ((i, wk_hbm), (2 + i, wv_hbm)):
                load(
                    ref.at[:, pl.ds((2 * i + j) * hd, hd)],
                    weights.at[j, ctx, :, pl.ds(at * hd, hd)],
                    j,
                )

    def load_q(j):
        for r in range(2):
            for i in range(2):
                load(
                    wq_hbm.at[:, pl.ds((4 * i + 2 * j + r) * hd, hd)],
                    weights.at[2 + j, ctx, :, pl.ds((2 * r + i) * hd, hd)],
                    2 + j,
                )

    load_kv(0)
    load(x_hbm, xv, 4)
    load(gain_hbm, gain_ref, 5)
    load(pos_hbm, pos_ref, 6)
    load(freq_hbm, freq_ref, 7)
    load_q(0)
    load_kv(1)
    load_q(1)
    loaded(weights.at[0, ctx], 0)
    pl.semaphore_wait(barrier, SHARDS + 1)

    sends = []

    def copy_of(src, dst, recv, dev, at):
        return pltpu.make_async_remote_copy(
            src_ref=src, dst_ref=dst, send_sem=send_sem.at[at % SENDS], recv_sem=recv,
            device_id=dev, device_id_type=MESH,
        )

    def sent(at):
        count, width = sends[at]
        ref = weights.at[0, 0, pl.ds(0, count), pl.ds(0, width)]
        copy_of(ref, ref, weight_sem.at[0, 0], to_peer, at).wait_send()

    def send(src, dst, recv, dev):
        if len(sends) >= SENDS:
            sent(len(sends) - SENDS)
        copy_of(src, dst, recv, dev, len(sends)).start()
        count, width = src.shape[-2:]
        sends.append((count * src.dtype.itemsize // 2, width))

    def await_copy(dst, recv):
        copy_of(dst, dst, recv, to_peer, 0).wait_recv()

    A, B = 0, 1
    own = ctx
    up_own, up_oth = up * 2 + par, up * 2 + other
    down_own, down_oth = down * 2 + par, down * 2 + other
    far_own, far_oth = far * 2 + par, far * 2 + other

    places = [(0, 0, nk), (2, 0, nk), (1, 0, nk), (3, 0, nk // 2), (3, nk // 2, nk // 2)]

    def add(p, *shards, first=False):
        buf, start, count = places[p]
        width = 256

        @pl.loop(0, count // width)
        def _(i):
            cols = pl.ds(pl.multiple_of(start + i * width, width), width)
            part = sum(
                jnp.dot(normed[s], weights[buf, s, :, cols], preferred_element_type=jnp.float32)
                for s in shards
            )
            acc[buf, :, cols] = part if first else acc[buf, :, cols] + part

    DN, UP, FAR, PAIR, DNO, UPO, FARO, PEER = 0, 2, 4, 5, 6, 7, 8, 9
    peer_role = [(down_own, 0), (up_own, 1), (far_own, 2), (pair, 3)]
    peer_role += [(down_oth, 4), (up_oth, 5), (far_oth, 6)]

    def part(p, shard, kind):
        base = core * (depth // 2) + (SPLITS[p] if kind else 0)
        size = depth // 2 - SPLITS[p] if kind else SPLITS[p]
        buf, start, count = places[p]
        return weights.at[buf, shard, pl.ds(pl.multiple_of(base, 16), size), pl.ds(start, count)]

    def side(p, shard, owner):
        at = pl.ds(pl.multiple_of(owner * (depth // 2), 16), depth // 2)
        buf, start, count = places[p]
        return weights.at[buf, shard, at, pl.ds(start, count)]

    def send_part(p, shard, kind, role, dev):
        ref = part(p, shard, kind)
        send(ref, ref, weight_sem.at[p, role], dev)

    def to_other_core(p, at):
        shard, role = peer_role[at]
        ref = side(p, shard, core)
        send(ref, ref, weight_sem.at[p, PEER + role], to_peer)

    def wait_part(p, shard, kind, role):
        await_copy(part(p, shard, kind), weight_sem.at[p, role])

    def wait_side(p, shard, role):
        await_copy(side(p, shard, core), weight_sem.at[p, role])

    to_y = (to_pair, to_cross)

    def a1(p):
        low, high = p % 2, 1 - p % 2
        wait_part(p, down_own, low, DN + low)
        send_part(p, down_own, low, FAR, to_up)
        send_part(p, down_own, low, DNO, to_y[low])
        wait_part(p, up_own, high, UP + high)
        send_part(p, up_own, high, FAR, to_down)
        send_part(p, up_own, high, UPO, to_y[high])

    def a2(p):
        low, high = p % 2, 1 - p % 2
        wait_part(p, down_own, high, DN + high)
        send_part(p, down_own, high, DNO, to_y[high])
        to_other_core(p, 0)
        wait_part(p, up_own, low, UP + low)
        send_part(p, up_own, low, UPO, to_y[low])
        to_other_core(p, 1)

    def a3(p):
        wait_side(p, far_own, FAR)
        send_part(p, far_own, A, FARO, to_pair)
        send_part(p, far_own, B, FARO, to_cross)
        to_other_core(p, 2)

    def y0(p):
        wait_side(p, pair, PAIR)
        to_other_core(p, 3)

    def y2(p):
        wait_side(p, down_oth, DNO)
        to_other_core(p, 4)
        wait_side(p, up_oth, UPO)
        to_other_core(p, 5)

    def y3(p):
        wait_side(p, far_oth, FARO)
        to_other_core(p, 6)

    def first_z(p):
        low, high = p % 2, 1 - p % 2
        send_part(p, own, low, DN + low, to_up)
        send_part(p, own, high, UP + high, to_down)

    def second_z(p):
        low, high = p % 2, 1 - p % 2
        send_part(p, own, high, DN + high, to_up)
        send_part(p, own, low, UP + low, to_down)

    def start_z(p):
        first_z(p)
        second_z(p)

    def start_y(p):
        send_part(p, own, A, PAIR, to_pair)
        send_part(p, own, B, PAIR, to_cross)

    def finish(p, *at):
        for i in at:
            shard, role = peer_role[i]
            await_copy(side(p, shard, 1 - core), weight_sem.at[p, PEER + role])
        add(p, *[peer_role[i][0] for i in at])

    dn_, up_, far_, pair_, dno_, upo_, faro_ = range(7)

    first_z(0)
    start_y(0)
    second_z(0)
    loaded(pos_ref, 6)
    posb[ctx] = jnp.broadcast_to(pos_ref[...].reshape(1, rows), (8, rows)).astype(jnp.float32)
    loaded(weights.at[2, ctx], 2)
    start_y(1)

    loaded(xv, 4)
    loaded(gain_ref, 5)
    loaded(freq_ref, 7)
    block = 64
    gain = gain_ref[...].reshape(1, feats)

    @pl.loop(0, rows // block)
    def _(i):
        at = tile(i, block)
        value = xv[at, :].astype(jnp.float32)
        scale = lax.rsqrt(jnp.mean(value * value, -1, keepdims=True) + 1e-06)
        out = (value * scale * gain).astype(jnp.bfloat16)
        for s in range(SHARDS):
            normed[s, at, :] = out[:, s * depth : (s + 1) * depth]

    loaded(weights.at[1, ctx], 1)
    loaded(weights.at[3, ctx], 3)

    def angles():
        angle = jnp.transpose(posb[ctx])[:, :1] * freq_ref[...]
        k = jnp.floor(angle * (2.0 / math.pi) + 0.5)
        t = angle - k * 1.5703125
        t = t - k * 4.8375129699707031e-4
        t = t - k * 7.5497899548918822e-8
        q = k - 4.0 * jnp.floor(k * 0.25)
        s = t * t
        sin = t + t * s * (-1.6666654611e-1 + s * (8.3321608736e-3 - s * 1.9515295891e-4))
        cos = 1.0 - 0.5 * s + s * s * (
            4.166664568298827e-2 + s * (s * 2.443315711809948e-5 - 1.388731625493765e-3)
        )
        odd = (q == 1.0) | (q == 3.0)
        sine = jnp.where(odd, cos, sin)
        cosine = jnp.where(odd, sin, cos)
        lane = lax.broadcasted_iota(jnp.int32, sine.shape, 1)
        sin_ref[...] = jnp.where((q >= 2.0) ^ (lane < hd // 2), -sine, sine)
        cos_ref[...] = jnp.where((q == 1.0) | (q == 2.0), -cosine, cosine)

    def rope(u):
        return u * cos_ref[...] + pltpu.roll(u, hd // 2, 1) * sin_ref[...]

    def keys_values(j):
        for ref, base in ((kvb.at[ctx], par), (kvx, other)):
            ref[j, :, :hd] = rope(acc[j, :, tile(base, hd)]).astype(jnp.bfloat16)
            ref[j, :, hd:] = acc[j, :, tile(2 + base, hd)].astype(jnp.bfloat16)

    def query(j, r):
        at = slice(r * rows, (r + 1) * rows)
        for ref, base in ((qx, other), (qb.at[0], par)):
            u = acc[2 + j, :, tile(2 * r + base, hd)]
            ref[j, at, :] = (rope(u) * query_scale).astype(jnp.bfloat16)
        send(qx.at[j, at, :], qb.at[1, j, at, :], q_sem.at[j, r], to_pair)

    def query_wait(j, r):
        at = slice(r * rows, (r + 1) * rows)
        await_copy(qb.at[1, j, at, :], q_sem.at[j, r])

    def kv_half(blk, j, half):
        return kvb.at[blk, j, pl.ds(half * half_rows, half_rows), :]

    def kv_send(blk, j, half, role, dev):
        ref = kv_half(blk, j, half)
        send(ref, ref, kv_sem.at[j, role], dev)

    def kv_to_pair(j):
        send(kvx.at[j], kvb.at[ctx, j], kv_sem.at[j, 0], to_pair)

    def kv_to_z(blk, j, base):
        for half in range(2):
            kv_send(blk, j, half, base + half, to_up)
            kv_send(blk, j, 1 - half, base + 2 + 1 - half, to_down)

    def kv_pair(j):
        await_copy(kvb.at[pair, j], kv_sem.at[j, 0])
        kv_to_z(pair, j, 6)

    def kv_relay(low, high, j, base):
        await_copy(kv_half(low, j, 0), kv_sem.at[j, base])
        kv_send(low, j, 0, base + 4, to_up)
        await_copy(kv_half(high, j, 1), kv_sem.at[j, base + 3])
        kv_send(high, j, 1, base + 4, to_down)
        await_copy(kv_half(low, j, 1), kv_sem.at[j, base + 1])
        await_copy(kv_half(high, j, 0), kv_sem.at[j, base + 2])

    def unit(src, j, step):
        zr = (z + step + step // 2 - 2 * (step // 3)) % 4
        blocks = pl.ds(zr * 2, 2)
        kk = kvb[blocks, j, :, :hd].reshape(2 * rows, hd)
        vv = kvb[blocks, j, :, hd:].reshape(2 * rows, hd)
        vv = jnp.concatenate([vv, jnp.ones_like(vv)], 1)
        kp = jnp.concatenate([posb[zr * 2, :1, :], posb[zr * 2 + 1, :1, :]], 1)
        s = lax.dot_general(
            qb[src, j], kk, (((1,), (1,)), ((), ())), preferred_element_type=jnp.float32
        )
        w = jnp.exp2(jnp.tanh(s * 0.02) * EXP_SCALE)
        w = jnp.where(kp <= qpos[src], w, 0.0).astype(jnp.bfloat16)
        num[src, j] += jnp.dot(w, vv, preferred_element_type=jnp.float32)

    def result(src, j, r):
        n = num[src, j, r * rows : (r + 1) * rows, :]
        return (n[:, :hd] / n[:, hd:]).astype(jnp.bfloat16)

    def columns(base, h):
        return o_hbm.at[:, tile(base * 4 + h, hd)]

    def give_back(j, r):
        h = 2 * j + r
        osend[h] = result(1, j, r)
        send(osend.at[h], columns(par, h), o_sem.at[0], to_pair)

    def keep(j, r):
        h = 2 * j + r
        oown[h] = result(0, j, r)
        pltpu.make_async_copy(oown.at[h], columns(par, h), out_sem.at[0]).start()

    def far_wait(j):
        await_copy(kvb.at[far_own, j], kv_sem.at[j, 5])
        await_copy(kvb.at[far_oth, j], kv_sem.at[j, 10])

    add(0, own, first=True)
    for dev in group:
        send(posb.at[ctx], posb.at[ctx], pos_sem.at[0], dev)
    angles()
    a1(0)
    start_z(1)
    y0(0)
    num[...] = jnp.zeros_like(num)
    a2(0)
    y0(1)
    finish(0, pair_)
    a3(0)
    finish(0, dn_, up_)
    a1(1)
    start_z(2)
    y2(0)
    add(1, own, first=True)
    finish(1, pair_)
    a2(1)
    y3(0)
    finish(0, dno_, upo_, far_)
    finish(0, faro_)
    keys_values(0)
    a3(1)
    kv_to_pair(0)
    kv_to_z(ctx, 0, 1)
    start_y(2)
    finish(1, dn_, up_)
    a1(2)
    start_z(3)
    y2(1)
    add(2, own, first=True)
    a2(2)
    await_copy(posb.at[pl.ds(0, SHARDS - 1)], pos_sem.at[0])
    for src, blk in ((0, ctx), (1, pair)):
        col = jnp.transpose(posb[blk])[:, :1]
        for r in range(2):
            qpos[src, r * rows : (r + 1) * rows, :] = col
    finish(1, dno_, upo_, far_)
    y3(1)
    finish(1, faro_)
    query(0, 0)
    query(0, 1)
    kv_relay(down_own, up_own, 0, 1)

    def before_0():
        kv_pair(0)

    def before_1():
        start_y(3)
        y0(2)
        a3(2)
        finish(2, pair_, dn_, up_)
        a1(3)
        a2(3)
        start_z(4)
        start_y(4)
        y2(2)
        finish(2, dno_, upo_, far_)
        query_wait(0, 0)
        query_wait(0, 1)

    def before_2():
        kv_relay(down_oth, up_oth, 0, 6)
        y0(3)

    def before_3():
        a3(3)
        y3(2)
        a1(4)
        finish(2, faro_)
        keys_values(1)
        kv_to_pair(1)
        kv_to_z(ctx, 1, 1)
        a2(4)

    def before_4():
        add(3, own, first=True)
        finish(3, pair_, dn_, up_)
        y2(3)

    def before_5():
        a3(4)
        y3(3)
        finish(3, dno_, upo_, far_)
        add(4, own, first=True)
        y0(4)
        finish(3, faro_)
        query(1, 0)
        finish(4, pair_, dn_, up_)
        y2(4)
        y3(4)
        kv_pair(1)
        finish(4, dno_, upo_, far_)
        finish(4, faro_)
        query(1, 1)

    def before_6():
        kv_relay(down_own, up_own, 1, 1)
        far_wait(0)

    def before_7():
        give_back(0, 0)
        give_back(0, 1)

    def before_8():
        keep(0, 0)
        keep(0, 1)

    def before_9():
        kv_relay(down_oth, up_oth, 1, 6)
        query_wait(1, 0)
        query_wait(1, 1)

    def before_13():
        give_back(1, 0)
        give_back(1, 1)

    before = {
        0: before_0, 1: before_1, 2: before_2, 3: before_3, 4: before_4, 5: before_5,
        6: before_6, 7: before_7, 8: before_8, 9: before_9,
        12: lambda: far_wait(1), 13: before_13,
    }

    @pl.loop(0, 16)
    def _(t):
        for at, action in before.items():
            pl.when(t == at)(action)
        j, u = t // 8, t % 8
        past = (u + 3) // 8
        late = (u + 3) // 4 - 2 * past
        theirs = (1 - j) * ((u % 2 + u // 6) % 2) + j * late
        unit(theirs, j, (1 - j) * (u // 2) + j * (u - late - 4 * past))

    keep(1, 0)
    keep(1, 1)
    mine = o_hbm.at[:, tile(par, 4 * hd)]
    pltpu.make_async_copy(mine, mine, out_sem.at[0]).wait()
    await_copy(o_hbm.at[:, tile(other, 4 * hd)], o_sem.at[0])
    for at in range(len(sends) - SENDS, len(sends)):
        sent(at)


def on_device(tokens, token_pos, norm_gain, query_weight, key_weight, value_weight):
    rows, feats = tokens.shape
    depth, nq = query_weight.shape
    nk = key_weight.shape[1]
    half = HEAD_DIM // 2
    freq = (10000.0 ** (-np.arange(half) * 2.0 / HEAD_DIM)).astype(np.float32)
    freq = jnp.asarray(np.concatenate([freq, freq])[None, :])
    hbm = pl.BlockSpec(memory_space=pl.ANY)
    bf16, f32 = jnp.bfloat16, jnp.float32
    dma = pltpu.SemaphoreType.DMA
    return pl.pallas_call(
        kernel,
        out_shape=jax.ShapeDtypeStruct((rows, nq), bf16),
        in_specs=[hbm] * 7,
        out_specs=hbm,
        scratch_shapes=[
            pltpu.VMEM((feats,), f32),
            pltpu.VMEM((1, HEAD_DIM), f32),
            pltpu.VMEM((rows,), jnp.int32),
            pltpu.VMEM((rows, HEAD_DIM), f32),
            pltpu.VMEM((rows, HEAD_DIM), f32),
            pltpu.VMEM((rows, feats), bf16),
            pltpu.VMEM((SHARDS, rows, depth), bf16),
            pltpu.VMEM((4, SHARDS, depth, nk), bf16),
            pltpu.VMEM((4, rows, nk), f32),
            pltpu.VMEM((SHARDS, 8, rows), f32),
            pltpu.VMEM((2, 2 * rows, 1), f32),
            pltpu.VMEM((SHARDS, 2, rows, 2 * HEAD_DIM), bf16),
            pltpu.VMEM((2, rows, 2 * HEAD_DIM), bf16),
            pltpu.VMEM((2, 2, 2 * rows, HEAD_DIM), bf16),
            pltpu.VMEM((2, 2 * rows, HEAD_DIM), bf16),
            pltpu.VMEM((2, 2, 2 * rows, 2 * HEAD_DIM), f32),
            pltpu.VMEM((4, rows, HEAD_DIM), bf16),
            pltpu.VMEM((4, rows, HEAD_DIM), bf16),
            dma((8,)),
            dma((1,)),
            dma((SENDS,)),
            dma((5, 16)),
            dma((2, 11)),
            dma((2, 2)),
            dma((1,)),
            dma((1,)),
        ],
        compiler_params=pltpu.CompilerParams(
            collective_id=0, has_side_effects=True, vmem_limit_bytes=62 * 1024 * 1024
        ),
        name="block",
    )(
        tokens, norm_gain, query_weight, key_weight, value_weight, freq, token_pos,
    )


def solution(mesh):
    in_specs = (
        P(("grp", "ctx"), None),
        P(("grp", "ctx")),
        P(),
        P("ctx", "tp"),
        P("ctx", "tp"),
        P("ctx", "tp"),
    )
    out_specs = P(("grp", "ctx"), "tp")
    return jax.shard_map(
        on_device, mesh=mesh, in_specs=in_specs, out_specs=out_specs, check_vma=False
    )
```
